256 devices in a mesh: groups: 2 (over y), space: 16 (over z), mp: 4 (over x), sub: 2 (over core).
Axes of the slice: x: 4, y: 2, z: 16, core: 2. Of those that a mesh axis runs over, the one named last changes fastest.
The devices are a block of a 4x16x16 slice.
Arguments:
- voxels: bfloat16 [98304, 512], P(('groups', 'space', 'sub')), parts along dimension 0, may hold values from -6 to 6
- window_ids: int32 [98304], P(('groups', 'space', 'sub')), parts along dimension 0, may hold values from 0 to 511, as said below
- voxel_slots: int32 [98304], P(('groups', 'space', 'sub')), parts along dimension 0, may hold values from 0 to 255, as said below
- window_counts: int32 [1024], P('groups'), parts along dimension 0, may hold values from 0 to 256, as said below
- norm_gain: float32 [512], replicated, may hold values from 0.25 to 1.75
- w_query_key: bfloat16 [2, 512, 512], P(None, None, 'mp'), may hold values from -2 to 2
- w_value: bfloat16 [512, 512], P(None, 'mp'), may hold values from -0.25 to 0.25
- w_out: bfloat16 [512, 512], P('mp'), may hold values from -0.25 to 0.25
- ffn_gain: float32 [512], replicated, may hold values from 0.25 to 1.75
- w_up: bfloat16 [512, 2048], P(None, 'mp'), may hold values from -0.25 to 0.25
- w_down: bfloat16 [2048, 512], P('mp'), may hold values from -0.125 to 0.125
Outputs:
- result: bfloat16 [98304, 512], P(('groups', 'space', 'sub'), 'mp'), parts along dimension 0
The draws below stay inside these ranges and needn't reach their ends.
There are 2 independent parts, one for each index of `groups`. The reference program is written for one: setup_inputs(seed, part) draws one part's arguments, and reference() takes and returns one part's arrays. A program takes and returns all parts, laid end to end along the dimension named above; an argument that names none is the same for every part. Nothing has to cross between parts.
Inputs may be any that keep to these rules, and one draw needn't show every extreme that they name: `window_ids`: window w belongs to owner w // 16 (its index along space+sub) as that owner's window w % 16. On the voxels of one device at most 96 lie in windows of one owner, and in every draw some owner has exactly 96 voxels of every device. `voxel_slots`: the voxels of a window hold slots 0 to its count - 1, each once. window_counts[w] is the number of voxels with window id w; some window holds 256.
All inputs are finite; a program needn't handle non-finite values.
Results may differ from the reference program's by a relative error of at most 0.012.
Values may be sent and summed in bfloat16 or wider, within the bound.
A program may use at most 64 MiB of HBM per device.

```python
import jax
import jax.numpy as jnp
from jax import lax

D = 512
HEADS = 8
HDIM = 64
FF = 2048
WLEN = 256
VOX_DEV = 1536
NOWN = 32
VOX = 49152
CAP = 96
WIN_DEV = 16
NWIN = 512


def scene(key):
    owner_total = NOWN
    capacity = CAP
    per_owner = WIN_DEV
    key_bias = jax.random.fold_in(key, 101)
    key_first = jax.random.fold_in(key, 102)
    key_score = jax.random.fold_in(key, 103)
    key_shuffle = jax.random.fold_in(key, 104)
    key_sizes = jax.random.fold_in(key, 105)
    bias = jax.random.randint(key_bias, (owner_total,), 0, 3)
    busiest = jax.random.randint(key_first, (), 0, owner_total)
    bias = jnp.where(jnp.arange(owner_total) == busiest, 3, bias)
    scores = jax.random.randint(key_score, (owner_total, owner_total, capacity), 0, 1 << 20) + (bias * (1 << 20))[None, :, None]
    scores = scores.reshape(owner_total, owner_total * capacity)
    chosen = jnp.argsort(-scores, axis=1, stable=True)[:, :VOX_DEV].astype(jnp.int32)
    source_ids = jnp.arange(owner_total, dtype=jnp.int32)[:, None]
    selected = jnp.zeros((owner_total, owner_total * capacity), jnp.int32).at[source_ids, chosen].set(1)
    shuffles = jax.vmap(lambda sub_key: jax.random.permutation(sub_key, VOX_DEV))(jax.random.split(key_shuffle, owner_total))
    slot_ids = jnp.take_along_axis(chosen, shuffles.astype(jnp.int32), axis=1)
    owner_of = slot_ids // capacity
    column_of = slot_ids % capacity
    by_owner = selected.reshape(owner_total, owner_total, capacity).transpose(1, 0, 2).reshape(owner_total, owner_total * capacity)
    earlier = (jnp.cumsum(by_owner, axis=1) - by_owner).reshape(owner_total, owner_total, capacity)
    rank_of = earlier[owner_of, jnp.broadcast_to(source_ids, owner_of.shape), column_of]
    sizes = jax.random.randint(key_sizes, (owner_total, per_owner), 3 * WLEN // 4, WLEN + 1)
    sizes = sizes.at[:, 0].set(WLEN)
    ends = jnp.cumsum(sizes, axis=1)
    starts = ends - sizes
    local_win = jnp.sum((rank_of[:, :, None] >= ends[owner_of]).astype(jnp.int32), axis=-1)
    slot_in = rank_of - jnp.take_along_axis(starts[owner_of], local_win[:, :, None], axis=-1)[:, :, 0]
    load = jnp.sum(selected.reshape(owner_total, owner_total, capacity), axis=(0, 2))
    counts_flat = jnp.clip(load[:, None] - starts, 0, sizes).reshape(-1)
    window_of = owner_of * per_owner + local_win
    return (window_of.reshape(-1).astype(jnp.int32), slot_in.reshape(-1).astype(jnp.int32), counts_flat.astype(jnp.int32))


def draw_window_ids(key, part):
    return scene(key)[0]


def draw_voxel_slots(key, part):
    return scene(key)[1]


def draw_window_counts(key, part):
    return scene(key)[2]


def draw_w_query_key(key, part):
    key_base = jax.random.fold_in(key, 201)
    stacked = jax.random.normal(key_base, (2, D, D), jnp.float32) * D ** (-0.5)
    return jnp.clip(stacked, -2.0, 2.0).astype(jnp.bfloat16)


def block_scale(rng, dims, pieces, low, high):
    factor_of, own = 1.0, jax.random.fold_in(rng, 6)
    for axis_at, shards_of in pieces:
        heights = jnp.exp(jax.random.uniform(jax.random.fold_in(own, axis_at), (shards_of,), jnp.float32, low / len(pieces), high / len(pieces)))
        factor_of = factor_of * jnp.repeat(heights, dims[axis_at] // shards_of).reshape([-1 if axis == axis_at else 1 for axis in range(len(dims))])
    return factor_of


def scatter_about(stream_key, dims, deviation, limit, pieces=(), kind=jnp.bfloat16):
    values = jax.random.normal(stream_key, dims, jnp.float32) * deviation
    if len(pieces) > 0:
        values = block_scale(stream_key, dims, pieces, -0.22, 0.18) * values
    return jnp.clip(values, min=-limit, max=limit).astype(kind)


def setup_inputs(seed: int = 0, part: int = 0) -> dict:
    splits = jax.random.split(jax.random.key(seed), 12)
    part_splits = jax.random.split(jax.random.fold_in(splits[11], part), 12)
    voxels = scatter_about(part_splits[0], (VOX, D), 1.0, 6.0, ((0, 32),))
    window_ids = draw_window_ids(jax.random.fold_in(jax.random.fold_in(splits[11], part), 71), part)
    voxel_slots = draw_voxel_slots(jax.random.fold_in(jax.random.fold_in(splits[11], part), 71), part)
    window_counts = draw_window_counts(jax.random.fold_in(jax.random.fold_in(splits[11], part), 71), part)
    norm_gain = jnp.clip(1.0 + 0.15 * jax.random.normal(splits[4], (D,), jnp.float32), 0.25, 1.75)
    w_query_key = draw_w_query_key(jax.random.fold_in(splits[11], 71), part)
    w_value = scatter_about(splits[6], (D, D), D ** -0.5, 0.25, ((1, 4),))
    w_out = scatter_about(splits[7], (D, D), D ** -0.5, 0.25, ((0, 4),))
    ffn_gain = jnp.clip(1.0 + 0.15 * jax.random.normal(splits[8], (D,), jnp.float32), 0.25, 1.75)
    w_up = scatter_about(splits[9], (D, FF), D ** -0.5, 0.25, ((1, 4),))
    w_down = scatter_about(splits[10], (FF, D), FF ** -0.5, 0.125, ((0, 4),))
    return dict(voxels=voxels, window_ids=window_ids, voxel_slots=voxel_slots, window_counts=window_counts, norm_gain=norm_gain, w_query_key=w_query_key, w_value=w_value, w_out=w_out, ffn_gain=ffn_gain, w_up=w_up, w_down=w_down)


def normalize(values_in, gain):
    row_mean = lax.optimization_barrier(jnp.mean(values_in, axis=-1, keepdims=True))
    centred = values_in - row_mean
    variance = lax.optimization_barrier(jnp.mean(centred * centred, axis=-1, keepdims=True))
    return centred * lax.rsqrt(variance + 1e-05) * gain.astype(jnp.float32)

def reference(voxels, window_ids, voxel_slots, window_counts, norm_gain, w_query_key, w_value, w_out, ffn_gain, w_up, w_down):
    stream = voxels.astype(jnp.float32)
    normed = normalize(stream, norm_gain).astype(jnp.bfloat16)
    queries = jnp.dot(normed, w_query_key[0], preferred_element_type=jnp.float32).astype(jnp.bfloat16)
    key_rows = jnp.dot(normed, w_query_key[1], preferred_element_type=jnp.float32).astype(jnp.bfloat16)
    values = jnp.dot(normed, w_value, preferred_element_type=jnp.float32).astype(jnp.bfloat16)
    flat_index = (window_ids * WLEN + voxel_slots).astype(jnp.int32)
    slot_table = jnp.zeros((NWIN * WLEN,), jnp.int32).at[flat_index].set(jnp.arange(VOX, dtype=jnp.int32))
    slot_table = slot_table.reshape(NWIN, WLEN)

    def one_window(operands):
        members, count = operands
        split_shape = (WLEN, HEADS, HDIM)
        window_q = queries[members].astype(jnp.float32).reshape(split_shape)
        window_k = key_rows[members].astype(jnp.float32).reshape(split_shape)
        window_v = values[members].astype(jnp.float32).reshape(split_shape)
        scores = jnp.einsum('qhd,khd->hqk', window_q, window_k, precision=lax.Precision.HIGHEST) * HDIM ** (-0.5)
        live_keys = jnp.arange(WLEN, dtype=jnp.int32) < count
        scores = jnp.where(live_keys[None, None, :], scores, jnp.float32(-1e+30))
        row_max = lax.optimization_barrier(jnp.max(scores, axis=-1, keepdims=True))
        weights = jnp.exp(scores - row_max)
        probabilities = (weights / lax.optimization_barrier(jnp.sum(weights, axis=-1, keepdims=True))).astype(jnp.bfloat16)
        mixture = jnp.einsum('hqk,khd->qhd', probabilities.astype(jnp.float32), window_v, precision=lax.Precision.HIGHEST)
        return mixture.astype(jnp.bfloat16).reshape(WLEN, D)
    windows_out = lax.map(one_window, (slot_table, window_counts))
    attended = windows_out.reshape(NWIN * WLEN, D)[flat_index]
    after_attn = stream + jnp.dot(attended, w_out, preferred_element_type=jnp.float32)
    normed_ffn = normalize(after_attn, ffn_gain).astype(jnp.bfloat16)
    hidden = jax.nn.gelu(jnp.dot(normed_ffn, w_up, preferred_element_type=jnp.float32), approximate=True).astype(jnp.bfloat16)
    return (after_attn + jnp.dot(hidden, w_down, preferred_element_type=jnp.float32)).astype(jnp.bfloat16)
```

```python
import functools

import jax
import jax.numpy as jnp
from jax import lax
from jax.experimental import pallas as pl
from jax.experimental.pallas import tpu as pltpu
from jax.sharding import PartitionSpec as P

HDIM = 64
WLEN = 256
WIN_DEV = 16
LANES = 128
MESH = pl.DeviceIdType.MESH
BF16 = jnp.bfloat16
F32 = jnp.float32


def dot(a, b):
    return jnp.dot(a, b, preferred_element_type=F32)


def dot_nt(a, b):
    return lax.dot_general(a, b, (((1,), (1,)), ((), ())), preferred_element_type=F32)


def dot_tn(a, b):
    return lax.dot_general(a, b, (((0,), (0,)), ((), ())), preferred_element_type=F32)


def pick(mask):
    return jnp.where(mask, 1.0, 0.0).astype(BF16)


def block_kernel(
    sizes,
    x_ref,
    ids_ref,
    slots_ref,
    counts_ref,
    gain_ref,
    wqk_ref,
    wv_ref,
    wo_ref,
    fgain_ref,
    wu_ref,
    wd_ref,
    out_ref,
    xn,
    packed,
    spot_out,
    spot_in,
    arr,
    spot_col,
    send_col,
    acc,
    mixt,
    ans,
    ret,
    att,
    attx,
    res,
    resx,
    wo_all,
    wu_all,
    wd_all,
    z_send,
    z_recv,
    s_send,
    s_recv,
    x_send,
    x_recv,
    b_send,
    b_recv,
    w_send,
    w_recv,
    d_send,
    d_recv,
    a_send,
    a_recv,
    r_send,
    r_recv,
):
    nz, nm, ns = sizes
    rows, width = x_ref.shape
    owners = nz * ns
    cap = 2 * rows // owners
    groups = nz // 2
    per = 2 * ns
    grows = per * cap
    quarter = rows // nm
    z = lax.axis_index("space")
    m = lax.axis_index("mp")
    s = lax.axis_index("sub")
    me = z * ns + s
    mcols = pl.ds(pl.multiple_of(m * LANES, LANES), LANES)

    def offset(g, j):
        if g == 0:
            return (0 if j < ns else nz // 2), j % ns
        return (g if j < ns else nz - g), j % ns

    def forward(g, j):
        dz, ds = offset(g, j)
        return lax.rem(z + dz, nz), lax.rem(s + ds, ns)

    def backward(g, j):
        dz, ds = offset(g, j)
        return lax.rem(z + (nz - dz), nz), lax.rem(s + ds, ns)

    def owner(g, j):
        tz, ts = forward(g, j)
        return tz * ns + ts

    def first(g):
        return 1 if g == 0 else 0

    def remote(src, dst, ssem, rsem, **where):
        return pltpu.make_async_remote_copy(
            src_ref=src,
            dst_ref=dst,
            send_sem=ssem,
            recv_sem=rsem,
            device_id=where,
            device_id_type=MESH,
        )

    order = [0] + list(range(groups - 1, 0, -1))
    others = [lax.rem(m + k, nm) for k in range(1, nm)]

    barrier = pltpu.get_barrier_semaphore()
    for g in range(groups):
        for j in range(first(g), per):
            tz, ts = forward(g, j)
            pl.semaphore_signal(
                barrier, inc=1, device_id={"space": tz, "sub": ts}, device_id_type=MESH
            )
    for om in others:
        pl.semaphore_signal(barrier, inc=1, device_id={"mp": om}, device_id_type=MESH)

    def norm_rows(i, carry):
        at = pl.ds(pl.multiple_of(i * 256, 256), 256)
        xb = x_ref[at, :].astype(F32)
        mean = jnp.sum(xb, axis=1, keepdims=True) * (1.0 / width)
        cen = xb - mean
        var = jnp.sum(cen * cen, axis=1, keepdims=True) * (1.0 / width)
        mine = x_ref[at, mcols].astype(F32) - mean
        xn[at, :] = (mine * lax.rsqrt(var + 1e-05) * gain_ref[:, mcols]).astype(BF16)
        return carry

    lax.fori_loop(0, rows // 256, norm_rows, 0)

    ids = ids_ref[...]
    dest = ids // WIN_DEV
    win = ids - dest * WIN_DEV
    owner_iota = lax.broadcasted_iota(jnp.int32, (owners, rows), 0)
    hit = owner_iota == dest
    table = pick(hit)
    step = 256
    earlier = pick(
        lax.broadcasted_iota(jnp.int32, (step, step), 0)
        < lax.broadcasted_iota(jnp.int32, (step, step), 1)
    )
    seen = jnp.zeros((owners, 1), F32)
    ranks = []
    for i in range(rows // step):
        part = table[:, i * step : (i + 1) * step]
        wide = part.astype(F32)
        before = dot(part, earlier) + seen
        ranks.append(jnp.sum(before * wide, axis=0, keepdims=True))
        seen = seen + jnp.sum(wide, axis=1, keepdims=True)
    rank = jnp.concatenate(ranks, axis=1).astype(jnp.int32)
    send = dest * cap + rank
    rank_hit = pick(lax.broadcasted_iota(jnp.int32, (LANES, rows), 0) == rank)
    slot_at = dot_nt(
        jnp.where(hit, (slots_ref[...] + 1).astype(F32), 0.0).astype(BF16), rank_hit
    )
    win_at = dot_nt(jnp.where(hit, win.astype(F32), 0.0).astype(BF16), rank_hit)
    spots = slot_at + win_at * float(WLEN)
    for o in range(owners):
        spot_out[o] = spots[o : o + 1, :]

    pl.semaphore_wait(barrier, groups * per - 1 + nm - 1)

    row_in = lax.broadcasted_iota(jnp.int32, (grows, 1), 0)
    lane_in = lax.broadcasted_iota(jnp.int32, (1, grows), 1)

    def places(g, inner):
        total = inner
        for j in range(per):
            low = owner(g, j) * cap - j * cap
            if j == 0:
                total = inner + low
            else:
                total = jnp.where(inner >= j * cap, inner + low, total)
        return total

    xn_all = xn[...]
    for g in order:
        for j in range(first(g), per):
            tz, ts = forward(g, j)
            remote(
                spot_out.at[owner(g, j)],
                spot_in.at[g, j],
                s_send.at[g],
                s_recv.at[g],
                space=tz,
                sub=ts,
            ).start()
        sel = pick(places(g, row_in) == send)
        packed[g] = dot(sel, xn_all).astype(BF16).reshape(per, cap, LANES)
        for j in range(first(g), per):
            tz, ts = forward(g, j)
            remote(
                packed.at[g, j],
                arr.at[g, j, :, mcols],
                z_send.at[g],
                z_recv.at[g],
                space=tz,
                sub=ts,
            ).start()

    arr[0, 0, :, mcols] = packed[0, 0]
    spot_in[0, 0] = spot_out[me]
    wo_all[m] = wo_ref[...]
    wu_all[m] = wu_ref[...]
    wd_all[m] = wd_ref[...]
    for i in range(rows // LANES):
        piece = send[:, i * LANES : (i + 1) * LANES].astype(F32)
        send_col[i * LANES : (i + 1) * LANES, :] = jnp.transpose(
            jnp.broadcast_to(piece, (LANES, LANES))
        )

    lane = lax.broadcasted_iota(jnp.int32, (1, LANES), 1)
    wqkv = jnp.concatenate([wqk_ref[0], wqk_ref[1], wv_ref[...]], axis=1)

    def spot_row(g):
        a0, a1, a2, a3 = (spot_in[g, j] for j in range(per))
        r1 = pltpu.roll(a1, 96, 1)
        r2 = pltpu.roll(a2, 64, 1)
        r3 = pltpu.roll(a3, 32, 1)
        t0 = a0 + jnp.where(lane >= 96, r1, 0.0)
        t1 = jnp.where(lane < 64, r1, 0.0) + jnp.where(lane >= 64, r2, 0.0)
        t2 = jnp.where(lane < 32, r2, 0.0) + jnp.where(lane >= 32, r3, 0.0)
        return [t0, t1, t2]

    def gather_wait(g):
        lo = first(g)
        remote(
            spot_out.at[pl.ds(0, per - lo)],
            spot_in.at[g, pl.ds(lo, per - lo)],
            s_send.at[g],
            s_recv.at[g],
            mp=others[0],
        ).wait_recv()
        remote(
            packed.at[g, pl.ds(lo, per - lo)],
            arr.at[g, pl.ds(lo, per - lo), :, mcols],
            z_send.at[g],
            z_recv.at[g],
            mp=others[0],
        ).wait_recv()

    def share(g, k):
        return remote(
            arr.at[g, :, :, mcols],
            arr.at[g, :, :, mcols],
            x_send.at[g, k],
            x_recv.at[g, k],
            mp=others[k],
        )

    def shared_wait(g):
        for k in range(nm - 1):
            share(g, k).wait_recv()

    def regroup(pair, fresh):
        parts = []
        for g in pair:
            tiles = spot_row(g)
            parts += tiles
            for i, t in enumerate(tiles):
                spot_col[g, i * LANES : (i + 1) * LANES, :] = jnp.transpose(
                    jnp.broadcast_to(t, (LANES, LANES))
                )
        row = jnp.concatenate(parts, axis=1).astype(jnp.int32)
        held = jnp.concatenate([arr[g].reshape(grows, width) for g in pair], axis=0)
        proj = dot(held, wqkv).astype(BF16)
        slot_iota = lax.broadcasted_iota(jnp.int32, (WLEN, row.shape[1]), 0) + 1

        def one_window(w, carry):
            got = dot(pick(slot_iota == row - w * WLEN), proj).astype(BF16)
            if fresh:
                acc[w] = got
            else:
                acc[w] = acc[w] + got
            return carry

        lax.fori_loop(0, WIN_DEV, one_window, 0)

    pairs = [order[i : i + 2] for i in range(0, groups, 2)]
    for i, pair in enumerate(pairs):
        for g in pair:
            gather_wait(g)
            for k in range(nm - 1):
                share(g, k).start()
        if i > 0:
            for g in pairs[i - 1]:
                shared_wait(g)
            regroup(pairs[i - 1], i == 1)

    def weight_parts(ref, all_ref, who):
        half = ref.shape[0] // ns
        at = pl.ds(pl.multiple_of(s * half, half), half)
        return ref.at[at], all_ref.at[who, at]

    def weight_copy(i, k):
        ref, all_ref = ((wu_ref, wu_all), (wd_ref, wd_all), (wo_ref, wo_all))[i]
        src, dst = weight_parts(ref, all_ref, m)
        return remote(src, dst, w_send.at[i, k], w_recv.at[i, k], mp=others[k])

    def weight_pass(i, k):
        ref, all_ref = ((wu_ref, wu_all), (wd_ref, wd_all), (wo_ref, wo_all))[i]
        src, dst = weight_parts(ref, all_ref, lax.rem(m + nm - 1 - k, nm))
        return remote(dst, dst, d_send.at[i, k], d_recv.at[i, k], sub=lax.rem(s + 1, ns))

    for i in range(3):
        for k in range(nm - 1):
            weight_copy(i, k).start()

    for g in pairs[-1]:
        shared_wait(g)
    regroup(pairs[-1], False)

    key_iota = lax.broadcasted_iota(jnp.int32, (WLEN, WLEN), 0)
    head_of = lax.broadcasted_iota(jnp.int32, (1, LANES), 1) // HDIM

    def attend(w, carry):
        here = acc[w]
        q = here[:, :LANES]
        k = here[:, LANES : 2 * LANES]
        v = here[:, 2 * LANES :]
        live = key_iota < counts_ref[me * WIN_DEV + w]
        parts = []
        vt = jnp.transpose(v.astype(F32)).astype(BF16)
        for h in range(LANES // HDIM):
            qh = jnp.where(head_of == h, q.astype(F32) * HDIM**-0.5, 0.0).astype(BF16)
            sc = jnp.where(live, dot_nt(k, qh), -1e30)
            weights = jnp.exp(sc - jnp.max(sc, axis=0, keepdims=True))
            total = jnp.sum(weights, axis=0, keepdims=True)
            mix = dot(vt[h * HDIM : (h + 1) * HDIM], weights.astype(BF16))
            parts.append(mix / total)
        at = pl.ds(pl.multiple_of(w * WLEN, WLEN), WLEN)
        mixt[:, at] = jnp.concatenate(parts, axis=0).astype(BF16)
        return carry

    lax.fori_loop(0, WIN_DEV, attend, 0)

    span = 4 * WLEN
    span_iota = lax.broadcasted_iota(jnp.int32, (1, span), 1)
    for g in order:
        col = spot_col[g].astype(jnp.int32)
        wide = jnp.concatenate([col] * (span // LANES), axis=1)

        def gather(c, total):
            at = pl.ds(pl.multiple_of(c * span, span), span)
            return total + dot_nt(pick(wide == span_iota + (c * span + 1)), mixt[:, at])

        total = lax.fori_loop(
            0, WIN_DEV * WLEN // span, gather, jnp.zeros((grows, LANES), F32)
        )
        ans[g] = total.astype(BF16).reshape(per, cap, LANES)
        for j in range(first(g), per):
            tz, ts = backward(g, j)
            remote(
                ans.at[g, j], ret.at[g, j], b_send.at[g], b_recv.at[g], space=tz, sub=ts
            ).start()
    ret[0, 0] = ans[0, 0]

    for i in range(3):
        for k in range(nm - 1):
            weight_copy(i, k).wait_recv()
            weight_pass(i, k).start()

    wide_send = send_col[...].astype(jnp.int32)
    wide_send = jnp.concatenate([wide_send] * (grows // LANES), axis=1)
    for n, g in enumerate(order):
        lo = first(g)
        remote(
            ans.at[g, pl.ds(lo, per - lo)],
            ret.at[g, pl.ds(lo, per - lo)],
            b_send.at[g],
            b_recv.at[g],
            mp=others[0],
        ).wait_recv()
        got = dot(
            pick(wide_send == places(g, lane_in)), ret[g].reshape(grows, LANES)
        ).astype(BF16)
        got = got.reshape(nm, quarter, LANES)
        if n == 0:
            att[...] = got
        else:
            att[...] = att[...] + got

    def head_copy(k):
        return remote(
            att.at[others[k]], attx.at[m], a_send.at[k], a_recv.at[k], mp=others[k]
        )

    for k in range(nm - 1):
        head_copy(k).start()
    attx[m] = att[m]
    for i in range(3):
        for k in range(nm - 1):
            weight_pass(i, k).wait_recv()
    for k in range(nm - 1):
        head_copy(k).wait_recv()

    heads = jnp.concatenate([attx[k] for k in range(nm)], axis=1)
    mine = pl.ds(pl.multiple_of(m * quarter, quarter), quarter)
    after = x_ref[mine, :].astype(F32) + dot(heads, wo_all[...].reshape(width, width))
    mean = jnp.sum(after, axis=1, keepdims=True) * (1.0 / width)
    cen = after - mean
    var = jnp.sum(cen * cen, axis=1, keepdims=True) * (1.0 / width)
    normed = (cen * lax.rsqrt(var + 1e-05) * fgain_ref[...]).astype(BF16)
    total = after
    for c in range(nm):
        up = dot(normed, wu_all[c])
        inner = 0.7978845608028654 * (up + 0.044715 * (up * up * up))
        hidden = (0.5 * up * (1.0 + jnp.tanh(inner))).astype(BF16)
        total = total + dot(hidden, wd_all[c])
    total = total.astype(BF16)
    for k in range(nm):
        res[k] = total[:, k * LANES : (k + 1) * LANES]

    def result_copy(k):
        return remote(
            res.at[others[k]], resx.at[m], r_send.at[k], r_recv.at[k], mp=others[k]
        )

    for k in range(nm - 1):
        result_copy(k).start()
    resx[m] = res[m]

    for g in range(groups):
        lo = first(g)
        at = pl.ds(lo, per - lo)
        remote(
            spot_out.at[pl.ds(0, per - lo)],
            spot_in.at[g, at],
            s_send.at[g],
            s_recv.at[g],
            mp=others[0],
        ).wait_send()
        remote(
            packed.at[g, at], arr.at[g, at, :, mcols], z_send.at[g], z_recv.at[g], mp=others[0]
        ).wait_send()
        remote(ans.at[g, at], ret.at[g, at], b_send.at[g], b_recv.at[g], mp=others[0]).wait_send()
        for k in range(nm - 1):
            share(g, k).wait_send()
    for k in range(nm - 1):
        for i in range(3):
            weight_copy(i, k).wait_send()
            weight_pass(i, k).wait_send()
        head_copy(k).wait_send()
        result_copy(k).wait_recv()
        result_copy(k).wait_send()
    out_ref[...] = resx[...].reshape(rows, LANES)


def shards(sizes, *args):
    x, ids, slots, counts, gain, wqk, wv, wo, fgain, wu, wd = args
    nz, nm, ns = sizes
    rows, width = x.shape
    owners = nz * ns
    cap = 2 * rows // owners
    groups = nz // 2
    per = 2 * ns
    grows = per * cap
    quarter = rows // nm
    vmem = pl.BlockSpec(memory_space=pltpu.VMEM)
    smem = pl.BlockSpec(memory_space=pltpu.SMEM)
    dma = pltpu.SemaphoreType.DMA
    return pl.pallas_call(
        functools.partial(block_kernel, sizes),
        out_shape=jax.ShapeDtypeStruct((rows, LANES), BF16),
        in_specs=[vmem, vmem, vmem, smem] + [vmem] * 7,
        out_specs=vmem,
        scratch_shapes=[
            pltpu.VMEM((rows, LANES), BF16),
            pltpu.VMEM((groups, per, cap, LANES), BF16),
            pltpu.VMEM((owners, 1, LANES), F32),
            pltpu.VMEM((groups, per, 1, LANES), F32),
            pltpu.VMEM((groups, per, cap, width), BF16),
            pltpu.VMEM((groups, grows, LANES), F32),
            pltpu.VMEM((rows, LANES), F32),
            pltpu.VMEM((WIN_DEV, WLEN, 3 * LANES), BF16),
            pltpu.VMEM((LANES, WIN_DEV * WLEN), BF16),
            pltpu.VMEM((groups, per, cap, LANES), BF16),
            pltpu.VMEM((groups, per, cap, LANES), BF16),
            pltpu.VMEM((nm, quarter, LANES), BF16),
            pltpu.VMEM((nm, quarter, LANES), BF16),
            pltpu.VMEM((nm, quarter, LANES), BF16),
            pltpu.VMEM((nm, quarter, LANES), BF16),
            pltpu.VMEM((nm,) + wo.shape, BF16),
            pltpu.VMEM((nm,) + wu.shape, BF16),
            pltpu.VMEM((nm,) + wd.shape, BF16),
            dma((groups,)),
            dma((groups,)),
            dma((groups,)),
            dma((groups,)),
            dma((groups, nm - 1)),
            dma((groups, nm - 1)),
            dma((groups,)),
            dma((groups,)),
            dma((3, nm - 1)),
            dma((3, nm - 1)),
            dma((3, nm - 1)),
            dma((3, nm - 1)),
            dma((nm - 1,)),
            dma((nm - 1,)),
            dma((nm - 1,)),
            dma((nm - 1,)),
        ],
        compiler_params=pltpu.CompilerParams(
            collective_id=0, has_side_effects=True, vmem_limit_bytes=60 * 1024 * 1024
        ),
        name="block",
    )(
        x,
        ids.reshape(1, rows),
        slots.reshape(1, rows),
        counts,
        gain.reshape(1, width),
        wqk,
        wv,
        wo,
        fgain.reshape(1, width),
        wu,
        wd,
    )


def solution(mesh):
    sizes = (mesh.shape["space"], mesh.shape["mp"], mesh.shape["sub"])
    return jax.shard_map(
        functools.partial(shards, sizes),
        mesh=mesh,
        in_specs=(
            P(("groups", "space", "sub"), None),
            P(("groups", "space", "sub")),
            P(("groups", "space", "sub")),
            P("groups"),
            P(),
            P(None, None, "mp"),
            P(None, "mp"),
            P("mp", None),
            P(),
            P(None, "mp"),
            P("mp", None),
        ),
        out_specs=P(("groups", "space", "sub"), "mp"),
        check_vma=False,
    )
```

```python
import functools

import jax
import jax.numpy as jnp
from jax import lax
from jax.experimental import pallas as pl
from jax.experimental.pallas import tpu as pltpu
from jax.sharding import PartitionSpec as P

HDIM = 64
CUTS = (2, 4, 6, 7)
FFN_CUTS = (2, 4, 6, 7)
WLEN = 256
WIN_DEV = 16
LANES = 128
MESH = pl.DeviceIdType.MESH
BF16 = jnp.bfloat16
F32 = jnp.float32


def dot(a, b):
    return jnp.dot(a, b, preferred_element_type=F32)


def dot_nt(a, b):
    return lax.dot_general(a, b, (((1,), (1,)), ((), ())), preferred_element_type=F32)


def dot_tn(a, b):
    return lax.dot_general(a, b, (((0,), (0,)), ((), ())), preferred_element_type=F32)


def pick(mask):
    return jnp.where(mask, 1.0, 0.0).astype(BF16)


def pick16(mask):
    return jnp.where(mask, jnp.ones((), BF16), jnp.zeros((), BF16))


def block_kernel(
    sizes,
    x_ref,
    ids_ref,
    slots_ref,
    counts_ref,
    gain_ref,
    wqk_ref,
    wv_ref,
    wo_ref,
    fgain_ref,
    wu_ref,
    wd_ref,
    out_ref,
    xn,
    packed,
    spot_out,
    spot_in,
    arr,
    spot_col,
    send_col,
    acc,
    mixt,
    ans,
    ret,
    xr,
    hx,
    res,
    rx,
    f_send,
    f_recv,
    wo_all,
    wu_all,
    wd_all,
    z_send,
    z_recv,
    s_send,
    s_recv,
    x_send,
    x_recv,
    b_send,
    b_recv,
    w_send,
    w_recv,
    v_send,
    v_recv,
    d_send,
    d_recv,
    a_send,
    a_recv,
    r_send,
    r_recv,
):
    nz, nm, ns = sizes
    rows, width = x_ref.shape
    owners = nz * ns
    cap = 2 * rows // owners
    groups = nz // 2
    per = 2 * ns
    grows = per * cap
    z = lax.axis_index("space")
    m = lax.axis_index("mp")
    s = lax.axis_index("sub")
    me = z * ns + s
    mcols = pl.ds(pl.multiple_of(m * LANES, LANES), LANES)

    def offset(g, j):
        if g == 0:
            return (0 if j < ns else nz // 2), j % ns
        return (g if j < ns else nz - g), j % ns

    def forward(g, j):
        dz, ds = offset(g, j)
        return lax.rem(z + dz, nz), lax.rem(s + ds, ns)

    def backward(g, j):
        dz, ds = offset(g, j)
        return lax.rem(z + (nz - dz), nz), lax.rem(s + ds, ns)

    def owner(g, j):
        tz, ts = forward(g, j)
        return tz * ns + ts

    def first(g):
        return 1 if g == 0 else 0

    def remote(src, dst, ssem, rsem, **where):
        return pltpu.make_async_remote_copy(
            src_ref=src,
            dst_ref=dst,
            send_sem=ssem,
            recv_sem=rsem,
            device_id=where,
            device_id_type=MESH,
        )

    order = []
    for g in range(1, groups // 2):
        order += [g, groups - g]
    order += [groups // 2, 0]
    uses = sorted(order, key=lambda g: (groups if g == 0 else g) + 0.5 * order.index(g))
    others = [lax.rem(m + k, nm) for k in range(1, nm)]

    barrier = pltpu.get_barrier_semaphore()
    for g in range(groups):
        for j in range(first(g), per):
            tz, ts = forward(g, j)
            pl.semaphore_signal(
                barrier, inc=1, device_id={"space": tz, "sub": ts}, device_id_type=MESH
            )
    for om in others:
        pl.semaphore_signal(barrier, inc=1, device_id={"mp": om}, device_id_type=MESH)

    def norm_rows(i, carry):
        at = pl.ds(pl.multiple_of(i * 256, 256), 256)
        xb = x_ref[at, :].astype(F32)
        mean = jnp.sum(xb, axis=1, keepdims=True) * (1.0 / width)
        cen = xb - mean
        var = jnp.sum(cen * cen, axis=1, keepdims=True) * (1.0 / width)
        mine = x_ref[at, mcols].astype(F32) - mean
        xn[at, :] = (mine * lax.rsqrt(var + 1e-05) * gain_ref[:, mcols]).astype(BF16)
        return carry

    lax.fori_loop(0, rows // 256, norm_rows, 0)

    ids = ids_ref[...]
    dest = ids // WIN_DEV
    win = ids - dest * WIN_DEV
    owner_iota = lax.broadcasted_iota(jnp.int32, (owners, rows), 0)
    hit = owner_iota == dest
    table = pick(hit)
    step = 256
    earlier = pick(
        lax.broadcasted_iota(jnp.int32, (step, step), 0)
        < lax.broadcasted_iota(jnp.int32, (step, step), 1)
    )
    seen = jnp.zeros((owners, 1), F32)
    ranks = []
    for i in range(rows // step):
        part = table[:, i * step : (i + 1) * step]
        wide = part.astype(F32)
        before = dot(part, earlier) + seen
        ranks.append(jnp.sum(before * wide, axis=0, keepdims=True))
        seen = seen + jnp.sum(wide, axis=1, keepdims=True)
    rank = jnp.concatenate(ranks, axis=1).astype(jnp.int32)
    send = dest * cap + rank
    rank_hit = pick(lax.broadcasted_iota(jnp.int32, (LANES, rows), 0) == rank)
    slot_at = dot_nt(
        jnp.where(hit, (slots_ref[...] + 1).astype(F32), 0.0).astype(BF16), rank_hit
    )
    win_at = dot_nt(jnp.where(hit, win.astype(F32), 0.0).astype(BF16), rank_hit)
    spots = slot_at + win_at * float(WLEN)
    for o in range(owners):
        spot_out[o] = spots[o : o + 1, :]

    pl.semaphore_wait(barrier, groups * per - 1 + nm - 1)

    row_in = lax.broadcasted_iota(jnp.int32, (grows, 1), 0)
    lane_in = lax.broadcasted_iota(jnp.int32, (1, grows), 1)

    def places(g, inner):
        total = inner
        for j in range(per):
            low = owner(g, j) * cap - j * cap
            if j == 0:
                total = inner + low
            else:
                total = jnp.where(inner >= j * cap, inner + low, total)
        return total

    xn_all = xn[...]
    for g in order:
        for j in range(first(g), per):
            tz, ts = forward(g, j)
            remote(
                spot_out.at[owner(g, j)],
                spot_in.at[g, j],
                s_send.at[g],
                s_recv.at[g],
                space=tz,
                sub=ts,
            ).start()
        sel = pick(places(g, row_in) == send)
        packed[g] = dot(sel, xn_all).astype(BF16).reshape(per, cap, LANES)
        for j in range(first(g), per):
            tz, ts = forward(g, j)
            remote(
                packed.at[g, j],
                arr.at[g, j, :, mcols],
                z_send.at[g],
                z_recv.at[g],
                space=tz,
                sub=ts,
            ).start()

    mine_iota = lax.broadcasted_iota(jnp.int32, (cap, 1), 0)

    def mine_of(g):
        near, far = (0, nz // 2) if g == 0 else (g, nz - g)
        tz = lax.rem(z + jnp.where(m < ns, near, far), nz)
        ts = lax.rem(s + lax.rem(m, ns), ns)
        return mine_iota + (tz * ns + ts) * cap

    def residual(part):
        at = jnp.concatenate([mine_of(g) for g in part], axis=0)
        got = dot(pick(at == send), x_ref[...]).astype(BF16)
        for n, g in enumerate(part):
            xr[g] = got[n * cap : (n + 1) * cap]

    arr[0, 0, :, mcols] = packed[0, 0]
    spot_in[0, 0] = spot_out[me]
    wo_all[m] = wo_ref[...]
    wu_all[m] = wu_ref[...]
    wd_all[m] = wd_ref[...]
    for i in range(rows // LANES):
        piece = send[:, i * LANES : (i + 1) * LANES].astype(F32)
        send_col[i * LANES : (i + 1) * LANES, :] = jnp.transpose(
            jnp.broadcast_to(piece, (LANES, LANES))
        )

    lane = lax.broadcasted_iota(jnp.int32, (1, LANES), 1)
    wqkv = jnp.concatenate([wqk_ref[0], wqk_ref[1], wv_ref[...]], axis=1)

    def spot_row(g):
        a0, a1, a2, a3 = (spot_in[g, j] for j in range(per))
        r1 = pltpu.roll(a1, 96, 1)
        r2 = pltpu.roll(a2, 64, 1)
        r3 = pltpu.roll(a3, 32, 1)
        t0 = a0 + jnp.where(lane >= 96, r1, 0.0)
        t1 = jnp.where(lane < 64, r1, 0.0) + jnp.where(lane >= 64, r2, 0.0)
        t2 = jnp.where(lane < 32, r2, 0.0) + jnp.where(lane >= 32, r3, 0.0)
        return [t0, t1, t2]

    def gather_wait(g):
        lo = first(g)
        remote(
            spot_out.at[pl.ds(0, per - lo)],
            spot_in.at[g, pl.ds(lo, per - lo)],
            s_send.at[g],
            s_recv.at[g],
            mp=others[0],
        ).wait_recv()
        remote(
            packed.at[g, pl.ds(lo, per - lo)],
            arr.at[g, pl.ds(lo, per - lo), :, mcols],
            z_send.at[g],
            z_recv.at[g],
            mp=others[0],
        ).wait_recv()

    sides = (lax.rem(m + 1, nm), lax.rem(m + nm - 1, nm))

    def cols(who):
        return pl.ds(pl.multiple_of(who * LANES, LANES), LANES)

    def share(g, side):
        ref = arr.at[g, :, :, mcols]
        return remote(ref, ref, x_send.at[g, side], x_recv.at[g, side], mp=sides[side])

    def share_on(g, side):
        half = pl.ds(side * (per // 2), per // 2)
        ref = arr.at[g, half, :, cols(sides[1 - side])]
        return remote(ref, ref, f_send.at[g, side], f_recv.at[g, side], mp=sides[side])

    def regroup(pair, fresh):
        parts = []
        for g in pair:
            tiles = spot_row(g)
            parts += tiles
            for i, t in enumerate(tiles):
                spot_col[g, i * LANES : (i + 1) * LANES, :] = jnp.transpose(
                    jnp.broadcast_to(t, (LANES, LANES))
                )
        row = jnp.concatenate(parts, axis=1).astype(jnp.int32) - 1
        row_win = row // WLEN
        row_slot = (row - row_win * WLEN).astype(F32)
        held = jnp.concatenate([arr[g].reshape(grows, width) for g in pair], axis=0)
        proj = dot(held, wqkv).astype(BF16)
        slot_iota = lax.broadcasted_iota(jnp.int32, (WLEN, row.shape[1]), 0).astype(F32).astype(BF16)
        few = 4

        def some_windows(i, carry):
            sels = []
            for n in range(few):
                key = jnp.where(row_win == i * few + n, row_slot, -1.0).astype(BF16)
                sels.append(pick16(slot_iota == key))
            got = dot(jnp.concatenate(sels, axis=0), proj).astype(BF16)
            at = pl.ds(pl.multiple_of(i * (few * WLEN), few * WLEN), few * WLEN)
            if fresh:
                acc[at, :] = got
            else:
                acc[at, :] = acc[at, :] + got
            return carry

        lax.fori_loop(0, WIN_DEV // few, some_windows, 0)

    sets = [uses[a:b] for a, b in zip((0,) + CUTS, CUTS + (groups,))]

    def stage(i):
        if 0 <= i < groups:
            gather_wait(uses[i])
            for side in range(2):
                share(uses[i], side).start()

    def stage_on(i):
        if 0 <= i < groups:
            for side in range(2):
                share(uses[i], side).wait_recv()
                share_on(uses[i], side).start()

    def stage_use(i):
        for n, part in enumerate(sets):
            if 0 <= i < groups and part[-1] == uses[i]:
                for g in part:
                    for side in range(2):
                        share_on(g, side).wait_recv()
                regroup(part, n == 0)

    for i in range(groups):
        stage(i)
        stage_on(i - 1)
        stage_use(i - 2)
        if i in (2, 4):
            residual(uses[:groups // 2] if i == 2 else uses[groups // 2:])
    stage_on(groups - 1)

    kept = ((wu_ref, wu_all), (wd_ref, wd_all), (wo_ref, wo_all))

    def weight_copy(i, side):
        ref, all_ref = kept[i]
        half = ref.shape[0] // ns
        at = pl.ds(pl.multiple_of(s * half, half), half)
        return remote(
            ref.at[at], all_ref.at[m, at], w_send.at[i, side], w_recv.at[i, side], mp=sides[side]
        )

    def weight_on(i, side):
        ref, all_ref = kept[i]
        half = ref.shape[0] // ns
        low = half // 2
        at = pl.ds(pl.multiple_of(s * half + side * low, low), low)
        part = all_ref.at[sides[1 - side], at]
        return remote(part, part, v_send.at[i, side], v_recv.at[i, side], mp=sides[side])

    def weight_pass(i, k):
        ref, all_ref = kept[i]
        half = ref.shape[0] // ns
        at = pl.ds(pl.multiple_of(s * half, half), half)
        part = all_ref.at[others[k], at]
        return remote(part, part, d_send.at[i, k], d_recv.at[i, k], sub=lax.rem(s + 1, ns))

    def weights_on(side):
        for i in range(3):
            weight_copy(i, side).wait_recv()
            weight_on(i, side).start()

    for i in range(3):
        for side in range(2):
            weight_copy(i, side).start()

    stage_use(groups - 2)
    stage_use(groups - 1)

    key_iota = lax.broadcasted_iota(jnp.int32, (WLEN, LANES), 0)
    heads_here = LANES // HDIM
    head_of = lane // HDIM
    own = [jnp.where(head_of == h, 1.0, 0.0).astype(BF16) for h in range(heads_here)]
    extra = [jnp.where(lane == (heads_here - 1 - h) * HDIM, 1.0, 0.0) for h in range(heads_here)]
    ones = jnp.ones((16, WLEN), BF16)

    def attend(w, carry):
        at = pl.ds(pl.multiple_of(w * WLEN, WLEN), WLEN)
        here = acc[at, :]
        q = here[:, :LANES] * jnp.asarray(HDIM**-0.5, BF16)
        k = here[:, LANES : 2 * LANES]
        v = here[:, 2 * LANES :]
        dead = jnp.where(key_iota < counts_ref[me * WIN_DEV + w], 0.0, -1e30)
        parts = []
        vt = jnp.transpose(v.astype(F32)).astype(BF16)
        for h in range(heads_here):
            qh = q * own[h] + extra[h].astype(BF16)
            kh = k * own[h] + (dead * extra[h]).astype(BF16)
            sc = dot_nt(kh, qh)
            weights = jnp.exp(sc - jnp.max(sc, axis=0, keepdims=True)).astype(BF16)
            both = jnp.concatenate([vt[h * HDIM : (h + 1) * HDIM], ones], axis=0)
            mix = dot(both, weights)
            parts.append(mix[:HDIM] / mix[HDIM : HDIM + 1])
        mixt[:, at] = jnp.concatenate(parts, axis=0).astype(BF16)
        return carry

    lax.fori_loop(0, WIN_DEV, attend, 0, unroll=2)

    span = 4 * WLEN
    span_iota = lax.broadcasted_iota(jnp.int32, (1, span), 1)
    for n, g in enumerate(order):
        col = spot_col[g].astype(jnp.int32)
        wide = jnp.concatenate([col] * (span // LANES), axis=1)

        def gather(c, total):
            at = pl.ds(pl.multiple_of(c * span, span), span)
            return total + dot_nt(pick(wide == span_iota + (c * span + 1)), mixt[:, at])

        total = lax.fori_loop(
            0, WIN_DEV * WLEN // span, gather, jnp.zeros((grows, LANES), F32)
        )
        ans[g] = total.astype(BF16).reshape(per, cap, LANES)
        for j in range(first(g), per):
            tz, ts = backward(g, j)
            remote(
                ans.at[g, j], ret.at[g, j], b_send.at[g], b_recv.at[g], space=tz, sub=ts
            ).start()
        if n == 0:
            for side in range(2):
                weights_on(side)
    ret[0, 0] = ans[0, 0]

    for i in range(3):
        for side in range(2):
            weight_on(i, side).wait_recv()
        for k in range(nm - 1):
            weight_pass(i, k).start()

    def onward(g, k):
        return remote(
            ret.at[g, others[k]], hx.at[g, m], a_send.at[g, k], a_recv.at[g, k], mp=others[k]
        )

    def result_copy(g, k):
        return remote(
            res.at[g, others[k]], rx.at[g, m], r_send.at[g, k], r_recv.at[g, k], mp=others[k]
        )

    def come_back(i):
        g = uses[i]
        at = pl.ds(first(g), per - first(g))
        remote(
            ans.at[g, at], ret.at[g, at], b_send.at[g], b_recv.at[g], mp=others[0]
        ).wait_recv()
        for k in range(nm - 1):
            onward(g, k).start()
        hx[g, m] = ret[g, m]

    def feed_forward(part):
        for g in part:
            for k in range(nm - 1):
                onward(g, k).wait_recv()
        heads = jnp.concatenate(
            [jnp.concatenate([hx[g, k] for k in range(nm)], axis=1) for g in part], axis=0
        )
        stream = jnp.concatenate([xr[g] for g in part], axis=0).astype(F32)
        after = stream + dot(heads, wo_all[...].reshape(width, width))
        mean = jnp.sum(after, axis=1, keepdims=True) * (1.0 / width)
        cen = after - mean
        var = jnp.sum(cen * cen, axis=1, keepdims=True) * (1.0 / width)
        normed = (cen * lax.rsqrt(var + 1e-05) * fgain_ref[...]).astype(BF16)
        total = after
        for c in range(nm):
            up = dot(normed, wu_all[c])
            inner = 0.7978845608028654 * (up + 0.044715 * (up * up * up))
            hidden = (0.5 * up * (1.0 + jnp.tanh(inner))).astype(BF16)
            total = total + dot(hidden, wd_all[c])
        total = total.astype(BF16)
        for n, g in enumerate(part):
            for k in range(nm):
                res[g, k] = total[n * cap : (n + 1) * cap, k * LANES : (k + 1) * LANES]
            for k in range(nm - 1):
                result_copy(g, k).start()
            rx[g, m] = res[g, m]

    wide_send = send_col[...].astype(jnp.int32)
    wide_send = jnp.concatenate([wide_send] * (grows // LANES), axis=1)

    def finish(g, fresh):
        for k in range(nm - 1):
            result_copy(g, k).wait_recv()
        got = dot(
            pick(wide_send == places(g, lane_in)), rx[g].reshape(grows, LANES)
        ).astype(BF16)
        if fresh:
            out_ref[...] = got
        else:
            out_ref[...] = out_ref[...] + got

    ffn_sets = [uses[a:b] for a, b in zip((0,) + FFN_CUTS, FFN_CUTS + (groups,))]
    ready = []
    for i in range(groups + 1):
        if i < groups:
            come_back(i)
        for part in ffn_sets:
            if i > 0 and part[-1] == uses[i - 1]:
                if i == 2:
                    for a in range(3):
                        for k in range(nm - 1):
                            weight_pass(a, k).wait_recv()
                feed_forward(part)
                for g in ready:
                    finish(g, g == uses[0])
                ready = part
    for g in ready:
        finish(g, False)

    for g in range(groups):
        lo = first(g)
        at = pl.ds(lo, per - lo)
        remote(
            spot_out.at[pl.ds(0, per - lo)],
            spot_in.at[g, at],
            s_send.at[g],
            s_recv.at[g],
            mp=others[0],
        ).wait_send()
        remote(
            packed.at[g, at], arr.at[g, at, :, mcols], z_send.at[g], z_recv.at[g], mp=others[0]
        ).wait_send()
        remote(ans.at[g, at], ret.at[g, at], b_send.at[g], b_recv.at[g], mp=others[0]).wait_send()
        for side in range(2):
            share(g, side).wait_send()
            share_on(g, side).wait_send()
        for k in range(nm - 1):
            onward(g, k).wait_send()
            result_copy(g, k).wait_send()
    for i in range(3):
        for side in range(2):
            weight_copy(i, side).wait_send()
            weight_on(i, side).wait_send()
        for k in range(nm - 1):
            weight_pass(i, k).wait_send()


def shards(sizes, *args):
    x, ids, slots, counts, gain, wqk, wv, wo, fgain, wu, wd = args
    nz, nm, ns = sizes
    rows, width = x.shape
    owners = nz * ns
    cap = 2 * rows // owners
    groups = nz // 2
    per = 2 * ns
    grows = per * cap
    vmem = pl.BlockSpec(memory_space=pltpu.VMEM)
    smem = pl.BlockSpec(memory_space=pltpu.SMEM)
    dma = pltpu.SemaphoreType.DMA
    return pl.pallas_call(
        functools.partial(block_kernel, sizes),
        out_shape=jax.ShapeDtypeStruct((rows, LANES), BF16),
        in_specs=[vmem, vmem, vmem, smem] + [vmem] * 7,
        out_specs=vmem,
        scratch_shapes=[
            pltpu.VMEM((rows, LANES), BF16),
            pltpu.VMEM((groups, per, cap, LANES), BF16),
            pltpu.VMEM((owners, 1, LANES), F32),
            pltpu.VMEM((groups, per, 1, LANES), F32),
            pltpu.VMEM((groups, per, cap, width), BF16),
            pltpu.VMEM((groups, grows, LANES), F32),
            pltpu.VMEM((rows, LANES), F32),
            pltpu.VMEM((WIN_DEV * WLEN, 3 * LANES), BF16),
            pltpu.VMEM((LANES, WIN_DEV * WLEN), BF16),
            pltpu.VMEM((groups, per, cap, LANES), BF16),
            pltpu.VMEM((groups, per, cap, LANES), BF16),
            pltpu.VMEM((groups, cap, width), BF16),
            pltpu.VMEM((groups, nm, cap, LANES), BF16),
            pltpu.VMEM((groups, nm, cap, LANES), BF16),
            pltpu.VMEM((groups, nm, cap, LANES), BF16),
            dma((groups, 2)),
            dma((groups, 2)),
            pltpu.VMEM((nm,) + wo.shape, BF16),
            pltpu.VMEM((nm,) + wu.shape, BF16),
            pltpu.VMEM((nm,) + wd.shape, BF16),
            dma((groups,)),
            dma((groups,)),
            dma((groups,)),
            dma((groups,)),
            dma((groups, 2)),
            dma((groups, 2)),
            dma((groups,)),
            dma((groups,)),
            dma((3, 2)),
            dma((3, 2)),
            dma((3, 2)),
            dma((3, 2)),
            dma((3, nm - 1)),
            dma((3, nm - 1)),
            dma((groups, nm - 1)),
            dma((groups, nm - 1)),
            dma((groups, nm - 1)),
            dma((groups, nm - 1)),
        ],
        compiler_params=pltpu.CompilerParams(
            collective_id=0, has_side_effects=True, vmem_limit_bytes=60 * 1024 * 1024
        ),
        name="block",
    )(
        x,
        ids.reshape(1, rows),
        slots.reshape(1, rows),
        counts,
        gain.reshape(1, width),
        wqk,
        wv,
        wo,
        fgain.reshape(1, width),
        wu,
        wd,
    )


def solution(mesh):
    sizes = (mesh.shape["space"], mesh.shape["mp"], mesh.shape["sub"])
    return jax.shard_map(
        functools.partial(shards, sizes),
        mesh=mesh,
        in_specs=(
            P(("groups", "space", "sub"), None),
            P(("groups", "space", "sub")),
            P(("groups", "space", "sub")),
            P("groups"),
            P(),
            P(None, None, "mp"),
            P(None, "mp"),
            P("mp", None),
            P(),
            P(None, "mp"),
            P("mp", None),
        ),
        out_specs=P(("groups", "space", "sub"), "mp"),
        check_vma=False,
    )
```

```python
import functools

import jax
import jax.numpy as jnp
from jax import lax
from jax.experimental import pallas as pl
from jax.experimental.pallas import tpu as pltpu
from jax.sharding import PartitionSpec as P

HDIM = 64
CUTS = (1, 2, 3, 4, 5, 6, 7)
AHEAD = 8
BACK = 8
FFN_CUTS = (2, 4, 6, 7)
WLEN = 256
WIN_DEV = 16
LANES = 128
MESH = pl.DeviceIdType.MESH
BF16 = jnp.bfloat16
F32 = jnp.float32


def dot(a, b):
    return jnp.dot(a, b, preferred_element_type=F32)


def dot_nt(a, b):
    return lax.dot_general(a, b, (((1,), (1,)), ((), ())), preferred_element_type=F32)


def dot_tn(a, b):
    return lax.dot_general(a, b, (((0,), (0,)), ((), ())), preferred_element_type=F32)


def pick(mask):
    return jnp.where(mask, 1.0, 0.0).astype(BF16)


def pick16(mask):
    return jnp.where(mask, jnp.ones((), BF16), jnp.zeros((), BF16))


def block_kernel(
    sizes,
    x_ref,
    ids_ref,
    slots_ref,
    counts_ref,
    gain_ref,
    wqk_ref,
    wv_ref,
    wo_ref,
    fgain_ref,
    wu_ref,
    wd_ref,
    out_ref,
    xn,
    packed,
    spot_out,
    spot_in,
    arr,
    spot_col,
    send_col,
    acc,
    mixt,
    ans,
    ret,
    sc_even,
    sc_odd,
    xr,
    hx,
    res,
    rx,
    f_send,
    f_recv,
    wo_all,
    wu_all,
    wd_all,
    z_send,
    z_recv,
    s_send,
    s_recv,
    x_send,
    x_recv,
    b_send,
    b_recv,
    w_send,
    w_recv,
    v_send,
    v_recv,
    d_send,
    d_recv,
    a_send,
    a_recv,
    r_send,
    r_recv,
):
    nz, nm, ns = sizes
    rows, width = x_ref.shape
    owners = nz * ns
    cap = 2 * rows // owners
    groups = nz // 2
    per = 2 * ns
    grows = per * cap
    z = lax.axis_index("space")
    m = lax.axis_index("mp")
    s = lax.axis_index("sub")
    me = z * ns + s
    mcols = pl.ds(pl.multiple_of(m * LANES, LANES), LANES)

    def offset(g, j):
        if g == 0:
            return (0 if j < ns else nz // 2), j % ns
        return (g if j < ns else nz - g), j % ns

    def forward(g, j):
        dz, ds = offset(g, j)
        return lax.rem(z + dz, nz), lax.rem(s + ds, ns)

    def backward(g, j):
        dz, ds = offset(g, j)
        return lax.rem(z + (nz - dz), nz), lax.rem(s + ds, ns)

    def owner(g, j):
        tz, ts = forward(g, j)
        return tz * ns + ts

    def first(g):
        return 1 if g == 0 else 0

    def remote(src, dst, ssem, rsem, **where):
        return pltpu.make_async_remote_copy(
            src_ref=src,
            dst_ref=dst,
            send_sem=ssem,
            recv_sem=rsem,
            device_id=where,
            device_id_type=MESH,
        )

    order = list(range(1, groups)) + [0]
    uses = order
    others = [lax.rem(m + k, nm) for k in range(1, nm)]

    barrier = pltpu.get_barrier_semaphore()
    for g in range(groups):
        for j in range(first(g), per):
            tz, ts = forward(g, j)
            pl.semaphore_signal(
                barrier, inc=1, device_id={"space": tz, "sub": ts}, device_id_type=MESH
            )
    for om in others:
        pl.semaphore_signal(barrier, inc=1, device_id={"mp": om}, device_id_type=MESH)

    def norm_rows(i, carry):
        at = pl.ds(pl.multiple_of(i * 256, 256), 256)
        xb = x_ref[at, :].astype(F32)
        mean = jnp.sum(xb, axis=1, keepdims=True) * (1.0 / width)
        cen = xb - mean
        var = jnp.sum(cen * cen, axis=1, keepdims=True) * (1.0 / width)
        mine = x_ref[at, mcols].astype(F32) - mean
        xn[at, :] = (mine * lax.rsqrt(var + 1e-05) * gain_ref[:, mcols]).astype(BF16)
        return carry

    lax.fori_loop(0, rows // 256, norm_rows, 0)

    ids = ids_ref[...].reshape(1, rows)
    dest = ids // WIN_DEV
    win = ids - dest * WIN_DEV
    owner_iota = lax.broadcasted_iota(jnp.int32, (owners, rows), 0)
    hit = owner_iota == dest
    table = pick(hit)
    step = 256
    earlier = pick(
        lax.broadcasted_iota(jnp.int32, (step, step), 0)
        < lax.broadcasted_iota(jnp.int32, (step, step), 1)
    )
    seen = jnp.zeros((owners, 1), F32)
    ranks = []
    for i in range(rows // step):
        part = table[:, i * step : (i + 1) * step]
        wide = part.astype(F32)
        before = dot(part, earlier) + seen
        ranks.append(jnp.sum(before * wide, axis=0, keepdims=True))
        seen = seen + jnp.sum(wide, axis=1, keepdims=True)
    rank = jnp.concatenate(ranks, axis=1).astype(jnp.int32)
    send = dest * cap + rank
    rank_hit = pick(lax.broadcasted_iota(jnp.int32, (LANES, rows), 0) == rank)
    slot_at = dot_nt(
        jnp.where(hit, (slots_ref[...].reshape(1, rows) + 1).astype(F32), 0.0).astype(BF16), rank_hit
    )
    win_at = dot_nt(jnp.where(hit, win.astype(F32), 0.0).astype(BF16), rank_hit)
    spots = slot_at + win_at * float(WLEN)
    for o in range(owners):
        spot_out[o] = spots[o : o + 1, :]

    pl.semaphore_wait(barrier, groups * per - 1 + nm - 1)

    row_in = lax.broadcasted_iota(jnp.int32, (grows, 1), 0)
    lane_in = lax.broadcasted_iota(jnp.int32, (1, grows), 1)

    def places(g, inner):
        total = inner
        for j in range(per):
            low = owner(g, j) * cap - j * cap
            if j == 0:
                total = inner + low
            else:
                total = jnp.where(inner >= j * cap, inner + low, total)
        return total

    for g in order:
        for j in range(first(g), per):
            tz, ts = forward(g, j)
            remote(
                spot_out.at[owner(g, j)],
                spot_in.at[g, j],
                s_send.at[g],
                s_recv.at[g],
                space=tz,
                sub=ts,
            ).start()

    def pack(g):
        sel = pick(places(g, row_in) == send)
        packed[g] = dot(sel, xn[...]).astype(BF16).reshape(per, cap, LANES)

    def post(i):
        if i < groups:
            g = order[i]
            for j in range(first(g), per):
                tz, ts = forward(g, j)
                remote(
                    packed.at[g, j],
                    arr.at[g, j, :, mcols],
                    z_send.at[g],
                    z_recv.at[g],
                    space=tz,
                    sub=ts,
                ).start()

    for i in range(groups):
        pack(order[i])
        if i < AHEAD:
            post(i)

    mine_iota = lax.broadcasted_iota(jnp.int32, (cap, 1), 0)

    def mine_of(g):
        near, far = (0, nz // 2) if g == 0 else (g, nz - g)
        tz = lax.rem(z + jnp.where(m < ns, near, far), nz)
        ts = lax.rem(s + lax.rem(m, ns), ns)
        return mine_iota + (tz * ns + ts) * cap

    def residual(part):
        at = jnp.concatenate([mine_of(g) for g in part], axis=0)
        got = dot(pick(at == send), x_ref[...]).astype(BF16)
        for n, g in enumerate(part):
            xr[g] = got[n * cap : (n + 1) * cap]

    arr[0, 0, :, mcols] = packed[0, 0]
    spot_in[0, 0] = spot_out[me]
    wo_all[m] = wo_ref[...]
    wu_all[m] = wu_ref[...]
    wd_all[m] = wd_ref[...]
    for i in range(rows // LANES):
        piece = send[:, i * LANES : (i + 1) * LANES].astype(F32)
        send_col[i * LANES : (i + 1) * LANES, :] = jnp.transpose(
            jnp.broadcast_to(piece, (LANES, LANES))
        )

    lane = lax.broadcasted_iota(jnp.int32, (1, LANES), 1)
    wqkv = jnp.concatenate([wqk_ref[0], wqk_ref[1], wv_ref[...]], axis=1)

    def spot_row(g):
        a0, a1, a2, a3 = (spot_in[g, j] for j in range(per))
        r1 = pltpu.roll(a1, 96, 1)
        r2 = pltpu.roll(a2, 64, 1)
        r3 = pltpu.roll(a3, 32, 1)
        t0 = a0 + jnp.where(lane >= 96, r1, 0.0)
        t1 = jnp.where(lane < 64, r1, 0.0) + jnp.where(lane >= 64, r2, 0.0)
        t2 = jnp.where(lane < 32, r2, 0.0) + jnp.where(lane >= 32, r3, 0.0)
        return [t0, t1, t2]

    def gather_wait(g):
        lo = first(g)
        remote(
            spot_out.at[pl.ds(0, per - lo)],
            spot_in.at[g, pl.ds(lo, per - lo)],
            s_send.at[g],
            s_recv.at[g],
            mp=others[0],
        ).wait_recv()
        remote(
            packed.at[g, pl.ds(lo, per - lo)],
            arr.at[g, pl.ds(lo, per - lo), :, mcols],
            z_send.at[g],
            z_recv.at[g],
            mp=others[0],
        ).wait_recv()

    sides = (lax.rem(m + 1, nm), lax.rem(m + nm - 1, nm))

    def cols(who):
        return pl.ds(pl.multiple_of(who * LANES, LANES), LANES)

    def share(g, side):
        ref = arr.at[g, :, :, mcols]
        return remote(ref, ref, x_send.at[g, side], x_recv.at[g, side], mp=sides[side])

    def share_on(g, side):
        half = pl.ds(side * (per // 2), per // 2)
        ref = arr.at[g, half, :, cols(sides[1 - side])]
        return remote(ref, ref, f_send.at[g, side], f_recv.at[g, side], mp=sides[side])

    def regroup(pair, fresh):
        parts = []
        for g in pair:
            tiles = spot_row(g)
            parts += tiles
            for i, t in enumerate(tiles):
                spot_col[g, i * LANES : (i + 1) * LANES, :] = jnp.transpose(
                    jnp.broadcast_to(t, (LANES, LANES))
                )
        row = jnp.concatenate(parts, axis=1).astype(jnp.int32) - 1
        row_win = row // WLEN
        row_slot = (row - row_win * WLEN).astype(F32)
        held = jnp.concatenate([arr[g].reshape(grows, width) for g in pair], axis=0)
        proj = dot(held, wqkv).astype(BF16)
        slot_iota = lax.broadcasted_iota(jnp.int32, (WLEN, row.shape[1]), 0).astype(F32).astype(BF16)
        few = 4

        def some_windows(i, carry):
            sels = []
            for n in range(few):
                key = jnp.where(row_win == i * few + n, row_slot, -1.0).astype(BF16)
                sels.append(pick16(slot_iota == key))
            got = dot(jnp.concatenate(sels, axis=0), proj).astype(BF16)
            at = pl.ds(pl.multiple_of(i * (few * WLEN), few * WLEN), few * WLEN)
            if fresh:
                acc[at, :] = got
            else:
                acc[at, :] = acc[at, :] + got
            return carry

        lax.fori_loop(0, WIN_DEV // few, some_windows, 0)

    sets = [uses[a:b] for a, b in zip((0,) + CUTS, CUTS + (groups,))]

    def stage(i):
        if 0 <= i < groups:
            gather_wait(uses[i])
            post(i + AHEAD)
            for side in range(2):
                share(uses[i], side).start()

    def stage_on(i):
        if 0 <= i < groups:
            for side in range(2):
                share(uses[i], side).wait_recv()
                share_on(uses[i], side).start()

    def stage_use(i):
        for n, part in enumerate(sets):
            if 0 <= i < groups and part[-1] == uses[i]:
                for g in part:
                    for side in range(2):
                        share_on(g, side).wait_recv()
                regroup(part, n == 0)

    for i in range(groups):
        stage(i)
        stage_use(i - 1)
        stage_on(i)
        if i in (2, 4):
            residual(uses[:groups // 2] if i == 2 else uses[groups // 2:])
    kept = ((wu_ref, wu_all), (wd_ref, wd_all), (wo_ref, wo_all))

    def weight_copy(i, side):
        ref, all_ref = kept[i]
        half = ref.shape[0] // ns
        at = pl.ds(pl.multiple_of(s * half, half), half)
        return remote(
            ref.at[at], all_ref.at[m, at], w_send.at[i, side], w_recv.at[i, side], mp=sides[side]
        )

    def weight_on(i, side):
        ref, all_ref = kept[i]
        half = ref.shape[0] // ns
        low = half // 2
        at = pl.ds(pl.multiple_of(s * half + side * low, low), low)
        part = all_ref.at[sides[1 - side], at]
        return remote(part, part, v_send.at[i, side], v_recv.at[i, side], mp=sides[side])

    def weight_pass(i, k):
        ref, all_ref = kept[i]
        half = ref.shape[0] // ns
        at = pl.ds(pl.multiple_of(s * half, half), half)
        part = all_ref.at[others[k], at]
        return remote(part, part, d_send.at[i, k], d_recv.at[i, k], sub=lax.rem(s + 1, ns))

    def weights_on(side):
        for i in range(3):
            weight_copy(i, side).wait_recv()
            weight_on(i, side).start()

    for i in range(3):
        for side in range(2):
            weight_copy(i, side).start()

    stage_use(groups - 1)

    key_iota = lax.broadcasted_iota(jnp.int32, (WLEN, LANES), 0)
    heads_here = LANES // HDIM
    head_of = lane // HDIM
    own = [jnp.where(head_of == h, 1.0, 0.0).astype(BF16) for h in range(heads_here)]
    extra = [jnp.where(lane == (heads_here - 1 - h) * HDIM, 1.0, 0.0) for h in range(heads_here)]
    ones = jnp.ones((16, WLEN), BF16)

    def score(w, sc_ref):
        here = acc[pl.ds(pl.multiple_of(w * WLEN, WLEN), WLEN), :]
        q = here[:, :LANES] * jnp.asarray(HDIM**-0.5, BF16)
        k = here[:, LANES : 2 * LANES]
        dead = jnp.where(key_iota < counts_ref[me * WIN_DEV + w], 0.0, -1e30)
        for h in range(heads_here):
            qh = q * own[h] + extra[h].astype(BF16)
            kh = k * own[h] + (dead * extra[h]).astype(BF16)
            sc_ref[h] = dot_nt(kh, qh)

    def mix(w, sc_ref):
        at = pl.ds(pl.multiple_of(w * WLEN, WLEN), WLEN)
        vt = jnp.transpose(acc[at, 2 * LANES :].astype(F32)).astype(BF16)
        parts = []
        for h in range(heads_here):
            sc = sc_ref[h]
            weights = jnp.exp(sc - jnp.max(sc, axis=0, keepdims=True)).astype(BF16)
            both = jnp.concatenate([vt[h * HDIM : (h + 1) * HDIM], ones], axis=0)
            got = dot(both, weights)
            parts.append(got[:HDIM] / got[HDIM : HDIM + 1])
        mixt[:, at] = jnp.concatenate(parts, axis=0).astype(BF16)

    def attend(i, carry):
        score(2 * i + 1, sc_odd)
        mix(2 * i, sc_even)
        score(jnp.minimum(2 * i + 2, WIN_DEV - 1), sc_even)
        mix(2 * i + 1, sc_odd)
        return carry

    score(0, sc_even)
    lax.fori_loop(0, WIN_DEV // 2, attend, 0)

    span = 4 * WLEN
    span_iota = lax.broadcasted_iota(jnp.int32, (1, span), 1)

    def answer(i):
        if i < groups:
            g = order[i]
            for j in range(first(g), per):
                tz, ts = backward(g, j)
                remote(
                    ans.at[g, j], ret.at[g, j], b_send.at[g], b_recv.at[g], space=tz, sub=ts
                ).start()

    for n, g in enumerate(order):
        col = spot_col[g].astype(jnp.int32)
        wide = jnp.concatenate([col] * (span // LANES), axis=1)

        def gather(c, total):
            at = pl.ds(pl.multiple_of(c * span, span), span)
            return total + dot_nt(pick(wide == span_iota + (c * span + 1)), mixt[:, at])

        total = lax.fori_loop(
            0, WIN_DEV * WLEN // span, gather, jnp.zeros((grows, LANES), F32)
        )
        ans[g] = total.astype(BF16).reshape(per, cap, LANES)
        if n < BACK:
            answer(n)
        if n == 0:
            for side in range(2):
                weights_on(side)
    ret[0, 0] = ans[0, 0]

    for i in range(3):
        for side in range(2):
            weight_on(i, side).wait_recv()
        for k in range(nm - 1):
            weight_pass(i, k).start()

    def onward(g, k):
        return remote(
            ret.at[g, others[k]], hx.at[g, m], a_send.at[g, k], a_recv.at[g, k], mp=others[k]
        )

    def result_copy(g, k):
        return remote(
            res.at[g, others[k]], rx.at[g, m], r_send.at[g, k], r_recv.at[g, k], mp=others[k]
        )

    def come_back(i):
        g = uses[i]
        at = pl.ds(first(g), per - first(g))
        remote(
            ans.at[g, at], ret.at[g, at], b_send.at[g], b_recv.at[g], mp=others[0]
        ).wait_recv()
        answer(i + BACK)
        for k in range(nm - 1):
            onward(g, k).start()
        hx[g, m] = ret[g, m]

    def feed_forward(part):
        for g in part:
            for k in range(nm - 1):
                onward(g, k).wait_recv()
        heads = jnp.concatenate(
            [jnp.concatenate([hx[g, k] for k in range(nm)], axis=1) for g in part], axis=0
        )
        stream = jnp.concatenate([xr[g] for g in part], axis=0).astype(F32)
        after = stream + dot(heads, wo_all[...].reshape(width, width))
        mean = jnp.sum(after, axis=1, keepdims=True) * (1.0 / width)
        cen = after - mean
        var = jnp.sum(cen * cen, axis=1, keepdims=True) * (1.0 / width)
        normed = (cen * lax.rsqrt(var + 1e-05) * fgain_ref[...]).astype(BF16)
        total = after
        for c in range(nm):
            up = dot(normed, wu_all[c])
            inner = 0.7978845608028654 * (up + 0.044715 * (up * up * up))
            hidden = (0.5 * up * (1.0 + jnp.tanh(inner))).astype(BF16)
            total = total + dot(hidden, wd_all[c])
        total = total.astype(BF16)
        for n, g in enumerate(part):
            for k in range(nm):
                res[g, k] = total[n * cap : (n + 1) * cap, k * LANES : (k + 1) * LANES]
            for k in range(nm - 1):
                result_copy(g, k).start()
            rx[g, m] = res[g, m]

    wide_send = send_col[...].astype(jnp.int32)
    wide_send = jnp.concatenate([wide_send] * (grows // LANES), axis=1)

    def finish(g, fresh):
        for k in range(nm - 1):
            result_copy(g, k).wait_recv()
        got = dot(
            pick(wide_send == places(g, lane_in)), rx[g].reshape(grows, LANES)
        ).astype(BF16)
        if fresh:
            out_ref[...] = got
        else:
            out_ref[...] = out_ref[...] + got

    ffn_sets = [uses[a:b] for a, b in zip((0,) + FFN_CUTS, FFN_CUTS + (groups,))]
    ready = []
    for i in range(groups + 1):
        if i < groups:
            come_back(i)
        for part in ffn_sets:
            if i > 0 and part[-1] == uses[i - 1]:
                if i == 2:
                    for a in range(3):
                        for k in range(nm - 1):
                            weight_pass(a, k).wait_recv()
                feed_forward(part)
                for g in ready:
                    finish(g, g == uses[0])
                ready = part
    for g in ready:
        finish(g, False)

    for g in range(groups):
        lo = first(g)
        at = pl.ds(lo, per - lo)
        remote(
            spot_out.at[pl.ds(0, per - lo)],
            spot_in.at[g, at],
            s_send.at[g],
            s_recv.at[g],
            mp=others[0],
        ).wait_send()
        remote(
            packed.at[g, at], arr.at[g, at, :, mcols], z_send.at[g], z_recv.at[g], mp=others[0]
        ).wait_send()
        remote(ans.at[g, at], ret.at[g, at], b_send.at[g], b_recv.at[g], mp=others[0]).wait_send()
        for side in range(2):
            share(g, side).wait_send()
            share_on(g, side).wait_send()
        for k in range(nm - 1):
            onward(g, k).wait_send()
            result_copy(g, k).wait_send()
    for i in range(3):
        for side in range(2):
            weight_copy(i, side).wait_send()
            weight_on(i, side).wait_send()
        for k in range(nm - 1):
            weight_pass(i, k).wait_send()


def shards(sizes, *args):
    x, ids, slots, counts, gain, wqk, wv, wo, fgain, wu, wd = args
    nz, nm, ns = sizes
    rows, width = x.shape
    owners = nz * ns
    cap = 2 * rows // owners
    groups = nz // 2
    per = 2 * ns
    grows = per * cap
    vmem = pl.BlockSpec(memory_space=pltpu.VMEM)
    smem = pl.BlockSpec(memory_space=pltpu.SMEM)
    dma = pltpu.SemaphoreType.DMA
    return pl.pallas_call(
        functools.partial(block_kernel, sizes),
        out_shape=jax.ShapeDtypeStruct((rows, LANES), BF16),
        in_specs=[vmem, vmem, vmem, smem] + [vmem] * 7,
        out_specs=vmem,
        scratch_shapes=[
            pltpu.VMEM((rows, LANES), BF16),
            pltpu.VMEM((groups, per, cap, LANES), BF16),
            pltpu.VMEM((owners, 1, LANES), F32),
            pltpu.VMEM((groups, per, 1, LANES), F32),
            pltpu.VMEM((groups, per, cap, width), BF16),
            pltpu.VMEM((groups, grows, LANES), F32),
            pltpu.VMEM((rows, LANES), F32),
            pltpu.VMEM((WIN_DEV * WLEN, 3 * LANES), BF16),
            pltpu.VMEM((LANES, WIN_DEV * WLEN), BF16),
            pltpu.VMEM((groups, per, cap, LANES), BF16),
            pltpu.VMEM((groups, per, cap, LANES), BF16),
            pltpu.VMEM((LANES // HDIM, WLEN, WLEN), F32),
            pltpu.VMEM((LANES // HDIM, WLEN, WLEN), F32),
            pltpu.VMEM((groups, cap, width), BF16),
            pltpu.VMEM((groups, nm, cap, LANES), BF16),
            pltpu.VMEM((groups, nm, cap, LANES), BF16),
            pltpu.VMEM((groups, nm, cap, LANES), BF16),
            dma((groups, 2)),
            dma((groups, 2)),
            pltpu.VMEM((nm,) + wo.shape, BF16),
            pltpu.VMEM((nm,) + wu.shape, BF16),
            pltpu.VMEM((nm,) + wd.shape, BF16),
            dma((groups,)),
            dma((groups,)),
            dma((groups,)),
            dma((groups,)),
            dma((groups, 2)),
            dma((groups, 2)),
            dma((groups,)),
            dma((groups,)),
            dma((3, 2)),
            dma((3, 2)),
            dma((3, 2)),
            dma((3, 2)),
            dma((3, nm - 1)),
            dma((3, nm - 1)),
            dma((groups, nm - 1)),
            dma((groups, nm - 1)),
            dma((groups, nm - 1)),
            dma((groups, nm - 1)),
        ],
        compiler_params=pltpu.CompilerParams(
            collective_id=0, has_side_effects=True, vmem_limit_bytes=60 * 1024 * 1024
        ),
        name="block",
    )(
        x,
        ids,
        slots,
        counts,
        gain.reshape(1, width),
        wqk,
        wv,
        wo,
        fgain.reshape(1, width),
        wu,
        wd,
    )


def solution(mesh):
    sizes = (mesh.shape["space"], mesh.shape["mp"], mesh.shape["sub"])
    return jax.shard_map(
        functools.partial(shards, sizes),
        mesh=mesh,
        in_specs=(
            P(("groups", "space", "sub"), None),
            P(("groups", "space", "sub")),
            P(("groups", "space", "sub")),
            P("groups"),
            P(),
            P(None, None, "mp"),
            P(None, "mp"),
            P("mp", None),
            P(),
            P(None, "mp"),
            P("mp", None),
        ),
        out_specs=P(("groups", "space", "sub"), "mp"),
        check_vma=False,
    )
```

```python
import functools

import jax
import jax.numpy as jnp
from jax import lax
from jax.experimental import pallas as pl
from jax.experimental.pallas import tpu as pltpu
from jax.sharding import PartitionSpec as P

HDIM = 64
CUTS = (1, 2, 3, 4, 5, 6, 7)
AHEAD = 8
BACK = 8
LAG = 3
FFN_CUTS = (2, 4, 6, 7)
WLEN = 256
WIN_DEV = 16
LANES = 128
MESH = pl.DeviceIdType.MESH
BF16 = jnp.bfloat16
F32 = jnp.float32


def dot(a, b):
    return jnp.dot(a, b, preferred_element_type=F32)


def dot_nt(a, b):
    return lax.dot_general(a, b, (((1,), (1,)), ((), ())), preferred_element_type=F32)


def dot_tn(a, b):
    return lax.dot_general(a, b, (((0,), (0,)), ((), ())), preferred_element_type=F32)


def pick(mask):
    return jnp.where(mask, 1.0, 0.0).astype(BF16)


def pick16(mask):
    return jnp.where(mask, jnp.ones((), BF16), jnp.zeros((), BF16))


def block_kernel(
    sizes,
    x_ref,
    ids_ref,
    slots_ref,
    counts_ref,
    gain_ref,
    wqk_ref,
    wv_ref,
    wo_ref,
    fgain_ref,
    wu_ref,
    wd_ref,
    out_ref,
    xn,
    packed,
    spot_out,
    spot_in,
    arr,
    spot_col,
    send_col,
    acc,
    mixt,
    ans,
    ret,
    sc_even,
    sc_odd,
    xr,
    hx,
    res,
    rx,
    f_send,
    f_recv,
    wo_all,
    wu_all,
    wd_all,
    z_send,
    z_recv,
    s_send,
    s_recv,
    x_send,
    x_recv,
    b_send,
    b_recv,
    w_send,
    w_recv,
    v_send,
    v_recv,
    d_send,
    d_recv,
    a_send,
    a_recv,
    r_send,
    r_recv,
):
    nz, nm, ns = sizes
    rows, width = x_ref.shape
    owners = nz * ns
    cap = 2 * rows // owners
    groups = nz // 2
    per = 2 * ns
    grows = per * cap
    z = lax.axis_index("space")
    m = lax.axis_index("mp")
    s = lax.axis_index("sub")
    me = z * ns + s
    mcols = pl.ds(pl.multiple_of(m * LANES, LANES), LANES)

    def offset(g, j):
        if g == 0:
            return (0 if j < ns else nz // 2), j % ns
        return (g if j < ns else nz - g), j % ns

    def forward(g, j):
        dz, ds = offset(g, j)
        return lax.rem(z + dz, nz), lax.rem(s + ds, ns)

    def backward(g, j):
        dz, ds = offset(g, j)
        return lax.rem(z + (nz - dz), nz), lax.rem(s + ds, ns)

    def owner(g, j):
        tz, ts = forward(g, j)
        return tz * ns + ts

    def first(g):
        return 1 if g == 0 else 0

    def remote(src, dst, ssem, rsem, **where):
        return pltpu.make_async_remote_copy(
            src_ref=src,
            dst_ref=dst,
            send_sem=ssem,
            recv_sem=rsem,
            device_id=where,
            device_id_type=MESH,
        )

    order = list(range(1, groups)) + [0]
    uses = order
    others = [lax.rem(m + k, nm) for k in range(1, nm)]

    barrier = pltpu.get_barrier_semaphore()
    for g in range(groups):
        for j in range(first(g), per):
            tz, ts = forward(g, j)
            pl.semaphore_signal(
                barrier, inc=1, device_id={"space": tz, "sub": ts}, device_id_type=MESH
            )
    for om in others:
        pl.semaphore_signal(barrier, inc=1, device_id={"mp": om}, device_id_type=MESH)

    def norm_rows(i, carry):
        at = pl.ds(pl.multiple_of(i * 256, 256), 256)
        xb = x_ref[at, :].astype(F32)
        mean = jnp.sum(xb, axis=1, keepdims=True) * (1.0 / width)
        cen = xb - mean
        var = jnp.sum(cen * cen, axis=1, keepdims=True) * (1.0 / width)
        mine = x_ref[at, mcols].astype(F32) - mean
        xn[at, :] = (mine * lax.rsqrt(var + 1e-05) * gain_ref[:, mcols]).astype(BF16)
        return carry

    lax.fori_loop(0, rows // 256, norm_rows, 0)

    ids = ids_ref[...].reshape(1, rows)
    dest = ids // WIN_DEV
    win = ids - dest * WIN_DEV
    owner_iota = lax.broadcasted_iota(jnp.int32, (owners, rows), 0)
    hit = owner_iota == dest
    table = pick(hit)
    step = 256
    earlier = pick(
        lax.broadcasted_iota(jnp.int32, (step, step), 0)
        < lax.broadcasted_iota(jnp.int32, (step, step), 1)
    )
    seen = jnp.zeros((owners, 1), F32)
    ranks = []
    for i in range(rows // step):
        part = table[:, i * step : (i + 1) * step]
        wide = part.astype(F32)
        before = dot(part, earlier) + seen
        ranks.append(jnp.sum(before * wide, axis=0, keepdims=True))
        seen = seen + jnp.sum(wide, axis=1, keepdims=True)
    rank = jnp.concatenate(ranks, axis=1).astype(jnp.int32)
    send = dest * cap + rank
    rank_hit = pick(lax.broadcasted_iota(jnp.int32, (LANES, rows), 0) == rank)
    slot_at = dot_nt(
        jnp.where(hit, (slots_ref[...].reshape(1, rows) + 1).astype(F32), 0.0).astype(BF16), rank_hit
    )
    win_at = dot_nt(jnp.where(hit, win.astype(F32), 0.0).astype(BF16), rank_hit)
    spots = slot_at + win_at * float(WLEN)
    for o in range(owners):
        spot_out[o] = spots[o : o + 1, :]

    pl.semaphore_wait(barrier, groups * per - 1 + nm - 1)

    row_in = lax.broadcasted_iota(jnp.int32, (grows, 1), 0)
    lane_in = lax.broadcasted_iota(jnp.int32, (1, grows), 1)

    def places(g, inner):
        total = inner
        for j in range(per):
            low = owner(g, j) * cap - j * cap
            if j == 0:
                total = inner + low
            else:
                total = jnp.where(inner >= j * cap, inner + low, total)
        return total

    for g in order:
        for j in range(first(g), per):
            tz, ts = forward(g, j)
            remote(
                spot_out.at[owner(g, j)],
                spot_in.at[g, j],
                s_send.at[g],
                s_recv.at[g],
                space=tz,
                sub=ts,
            ).start()

    def pack(g):
        sel = pick(places(g, row_in) == send)
        packed[g] = dot(sel, xn[...]).astype(BF16).reshape(per, cap, LANES)

    def post(i):
        if i < groups:
            g = order[i]
            for j in range(first(g), per):
                tz, ts = forward(g, j)
                remote(
                    packed.at[g, j],
                    arr.at[g, j, :, mcols],
                    z_send.at[g],
                    z_recv.at[g],
                    space=tz,
                    sub=ts,
                ).start()

    for i in range(groups):
        pack(order[i])
        if i < AHEAD:
            post(i)

    mine_iota = lax.broadcasted_iota(jnp.int32, (cap, 1), 0)

    def mine_of(g):
        near, far = (0, nz // 2) if g == 0 else (g, nz - g)
        tz = lax.rem(z + jnp.where(m < ns, near, far), nz)
        ts = lax.rem(s + lax.rem(m, ns), ns)
        return mine_iota + (tz * ns + ts) * cap

    def residual(part):
        at = jnp.concatenate([mine_of(g) for g in part], axis=0)
        got = dot(pick(at == send), x_ref[...]).astype(BF16)
        for n, g in enumerate(part):
            xr[g] = got[n * cap : (n + 1) * cap]

    arr[0, 0, :, mcols] = packed[0, 0]
    spot_in[0, 0] = spot_out[me]
    wo_all[m] = wo_ref[...]
    wu_all[m] = wu_ref[...]
    wd_all[m] = wd_ref[...]
    for i in range(rows // LANES):
        piece = send[:, i * LANES : (i + 1) * LANES].astype(F32)
        send_col[i * LANES : (i + 1) * LANES, :] = jnp.transpose(
            jnp.broadcast_to(piece, (LANES, LANES))
        )

    lane = lax.broadcasted_iota(jnp.int32, (1, LANES), 1)
    wqkv = jnp.concatenate([wqk_ref[0], wqk_ref[1], wv_ref[...]], axis=1)

    def spot_row(g):
        a0, a1, a2, a3 = (spot_in[g, j] for j in range(per))
        r1 = pltpu.roll(a1, 96, 1)
        r2 = pltpu.roll(a2, 64, 1)
        r3 = pltpu.roll(a3, 32, 1)
        t0 = a0 + jnp.where(lane >= 96, r1, 0.0)
        t1 = jnp.where(lane < 64, r1, 0.0) + jnp.where(lane >= 64, r2, 0.0)
        t2 = jnp.where(lane < 32, r2, 0.0) + jnp.where(lane >= 32, r3, 0.0)
        return [t0, t1, t2]

    def gather_wait(g):
        lo = first(g)
        remote(
            spot_out.at[pl.ds(0, per - lo)],
            spot_in.at[g, pl.ds(lo, per - lo)],
            s_send.at[g],
            s_recv.at[g],
            mp=others[0],
        ).wait_recv()
        remote(
            packed.at[g, pl.ds(lo, per - lo)],
            arr.at[g, pl.ds(lo, per - lo), :, mcols],
            z_send.at[g],
            z_recv.at[g],
            mp=others[0],
        ).wait_recv()

    sides = (lax.rem(m + 1, nm), lax.rem(m + nm - 1, nm))

    def cols(who):
        return pl.ds(pl.multiple_of(who * LANES, LANES), LANES)

    def share(g, side):
        ref = arr.at[g, :, :, mcols]
        return remote(ref, ref, x_send.at[g, side], x_recv.at[g, side], mp=sides[side])

    def share_on(g, side):
        half = pl.ds(side * (per // 2), per // 2)
        ref = arr.at[g, half, :, cols(sides[1 - side])]
        return remote(ref, ref, f_send.at[g, side], f_recv.at[g, side], mp=sides[side])

    def regroup(pair, fresh):
        parts = []
        for g in pair:
            tiles = spot_row(g)
            parts += tiles
            for i, t in enumerate(tiles):
                spot_col[g, i * LANES : (i + 1) * LANES, :] = jnp.transpose(
                    jnp.broadcast_to(t, (LANES, LANES))
                )
        row = jnp.concatenate(parts, axis=1).astype(jnp.int32) - 1
        row_win = row // WLEN
        row_slot = (row - row_win * WLEN).astype(F32)
        held = jnp.concatenate([arr[g].reshape(grows, width) for g in pair], axis=0)
        proj = dot(held, wqkv).astype(BF16)
        slot_iota = lax.broadcasted_iota(jnp.int32, (WLEN, row.shape[1]), 0).astype(F32).astype(BF16)
        few = 4

        def some_windows(i, carry):
            sels = []
            for n in range(few):
                key = jnp.where(row_win == i * few + n, row_slot, -1.0).astype(BF16)
                sels.append(pick16(slot_iota == key))
            got = dot(jnp.concatenate(sels, axis=0), proj).astype(BF16)
            at = pl.ds(pl.multiple_of(i * (few * WLEN), few * WLEN), few * WLEN)
            if fresh:
                acc[at, :] = got
            else:
                acc[at, :] = acc[at, :] + got
            return carry

        lax.fori_loop(0, WIN_DEV // few, some_windows, 0)

    kept = ((wu_ref, wu_all), (wd_ref, wd_all), (wo_ref, wo_all))

    def weight_copy(i, side):
        ref, all_ref = kept[i]
        half = ref.shape[0] // ns
        at = pl.ds(pl.multiple_of(s * half, half), half)
        return remote(
            ref.at[at], all_ref.at[m, at], w_send.at[i, side], w_recv.at[i, side], mp=sides[side]
        )

    def weight_on(i, side):
        ref, all_ref = kept[i]
        half = ref.shape[0] // ns
        low = half // 2
        at = pl.ds(pl.multiple_of(s * half + side * low, low), low)
        part = all_ref.at[sides[1 - side], at]
        return remote(part, part, v_send.at[i, side], v_recv.at[i, side], mp=sides[side])

    def weight_pass(i, k):
        ref, all_ref = kept[i]
        half = ref.shape[0] // ns
        at = pl.ds(pl.multiple_of(s * half, half), half)
        part = all_ref.at[others[k], at]
        return remote(part, part, d_send.at[i, k], d_recv.at[i, k], sub=lax.rem(s + 1, ns))

    def weights_out(i):
        for side in range(2):
            weight_copy(i, side).start()

    def weights_on(i):
        for side in range(2):
            weight_copy(i, side).wait_recv()
            weight_on(i, side).start()

    def weights_pass(i):
        for side in range(2):
            weight_on(i, side).wait_recv()
        for k in range(nm - 1):
            weight_pass(i, k).start()

    sets = [uses[a:b] for a, b in zip((0,) + CUTS, CUTS + (groups,))]

    def stage(i):
        if 0 <= i < groups:
            gather_wait(uses[i])
            post(i + AHEAD)
            for side in range(2):
                share(uses[i], side).start()

    def stage_on(i):
        if 0 <= i < groups:
            for side in range(2):
                share(uses[i], side).wait_recv()
                share_on(uses[i], side).start()

    def stage_use(i):
        for n, part in enumerate(sets):
            if 0 <= i < groups and part[-1] == uses[i]:
                for g in part:
                    for side in range(2):
                        share_on(g, side).wait_recv()
                regroup(part, n == 0)

    for i in range(groups):
        stage(i)
        stage_use(i - 1)
        stage_on(i)
        if i in (3, 4, 5):
            weights_out(i - 3)
        if i == 5:
            weights_on(0)
        if i == 6:
            weights_on(1)
            weights_on(2)
        if i in (2, 4):
            residual(uses[:groups // 2] if i == 2 else uses[groups // 2:])
    stage_use(groups - 1)

    key_iota = lax.broadcasted_iota(jnp.int32, (WLEN, LANES), 0)
    heads_here = LANES // HDIM
    head_of = lane // HDIM
    own = [jnp.where(head_of == h, 1.0, 0.0).astype(BF16) for h in range(heads_here)]
    extra = [jnp.where(lane == (heads_here - 1 - h) * HDIM, 1.0, 0.0) for h in range(heads_here)]
    ones = jnp.ones((16, WLEN), BF16)

    def score(w, sc_ref):
        here = acc[pl.ds(pl.multiple_of(w * WLEN, WLEN), WLEN), :]
        q = here[:, :LANES] * jnp.asarray(HDIM**-0.5, BF16)
        k = here[:, LANES : 2 * LANES]
        dead = jnp.where(key_iota < counts_ref[me * WIN_DEV + w], 0.0, -1e30)
        for h in range(heads_here):
            qh = q * own[h] + extra[h].astype(BF16)
            kh = k * own[h] + (dead * extra[h]).astype(BF16)
            sc_ref[h] = dot_nt(kh, qh)

    def mix(w, sc_ref):
        at = pl.ds(pl.multiple_of(w * WLEN, WLEN), WLEN)
        vt = jnp.transpose(acc[at, 2 * LANES :].astype(F32)).astype(BF16)
        parts = []
        for h in range(heads_here):
            sc = sc_ref[h]
            weights = jnp.exp(sc - jnp.max(sc, axis=0, keepdims=True)).astype(BF16)
            both = jnp.concatenate([vt[h * HDIM : (h + 1) * HDIM], ones], axis=0)
            got = dot(both, weights)
            parts.append(got[:HDIM] / got[HDIM : HDIM + 1])
        mixt[:, at] = jnp.concatenate(parts, axis=0).astype(BF16)

    def attend(i, carry):
        score(2 * i + 1, sc_odd)
        mix(2 * i, sc_even)
        score(jnp.minimum(2 * i + 2, WIN_DEV - 1), sc_even)
        mix(2 * i + 1, sc_odd)
        return carry

    score(0, sc_even)
    lax.fori_loop(0, WIN_DEV // 2, attend, 0)

    span = 4 * WLEN
    span_iota = lax.broadcasted_iota(jnp.int32, (1, span), 1)

    def answer(i):
        if i < groups:
            g = order[i]
            for j in range(first(g), per):
                tz, ts = backward(g, j)
                remote(
                    ans.at[g, j], ret.at[g, j], b_send.at[g], b_recv.at[g], space=tz, sub=ts
                ).start()

    def onward(g, k):
        return remote(
            ret.at[g, others[k]], hx.at[g, m], a_send.at[g, k], a_recv.at[g, k], mp=others[k]
        )

    def result_copy(g, k):
        return remote(
            res.at[g, others[k]], rx.at[g, m], r_send.at[g, k], r_recv.at[g, k], mp=others[k]
        )

    def come_back(i):
        g = uses[i]
        at = pl.ds(first(g), per - first(g))
        remote(
            ans.at[g, at], ret.at[g, at], b_send.at[g], b_recv.at[g], mp=others[0]
        ).wait_recv()
        answer(i + BACK)
        for k in range(nm - 1):
            onward(g, k).start()
        hx[g, m] = ret[g, m]

    for n, g in enumerate(order):
        col = spot_col[g].astype(jnp.int32)
        wide = jnp.concatenate([col] * (span // LANES), axis=1)

        def gather(c, total):
            at = pl.ds(pl.multiple_of(c * span, span), span)
            return total + dot_nt(pick(wide == span_iota + (c * span + 1)), mixt[:, at])

        total = lax.fori_loop(
            0, WIN_DEV * WLEN // span, gather, jnp.zeros((grows, LANES), F32)
        )
        ans[g] = total.astype(BF16).reshape(per, cap, LANES)
        if g == 0:
            ret[0, 0] = ans[0, 0]
        if n < BACK:
            answer(n)
        if n < 3:
            weights_pass(n)
        if n >= LAG:
            come_back(n - LAG)

    def feed_forward(part):
        for g in part:
            for k in range(nm - 1):
                onward(g, k).wait_recv()
        heads = jnp.concatenate(
            [jnp.concatenate([hx[g, k] for k in range(nm)], axis=1) for g in part], axis=0
        )
        stream = jnp.concatenate([xr[g] for g in part], axis=0).astype(F32)
        after = stream + dot(heads, wo_all[...].reshape(width, width))
        mean = jnp.sum(after, axis=1, keepdims=True) * (1.0 / width)
        cen = after - mean
        var = jnp.sum(cen * cen, axis=1, keepdims=True) * (1.0 / width)
        normed = (cen * lax.rsqrt(var + 1e-05) * fgain_ref[...]).astype(BF16)
        total = after
        for c in range(nm):
            up = dot(normed, wu_all[c])
            inner = 0.7978845608028654 * (up + 0.044715 * (up * up * up))
            hidden = (0.5 * up * (1.0 + jnp.tanh(inner))).astype(BF16)
            total = total + dot(hidden, wd_all[c])
        total = total.astype(BF16)
        for n, g in enumerate(part):
            for k in range(nm):
                res[g, k] = total[n * cap : (n + 1) * cap, k * LANES : (k + 1) * LANES]
            for k in range(nm - 1):
                result_copy(g, k).start()
            rx[g, m] = res[g, m]

    wide_send = send_col[...].astype(jnp.int32)
    wide_send = jnp.concatenate([wide_send] * (grows // LANES), axis=1)

    def finish(g, fresh):
        for k in range(nm - 1):
            result_copy(g, k).wait_recv()
        got = dot(
            pick(wide_send == places(g, lane_in)), rx[g].reshape(grows, LANES)
        ).astype(BF16)
        if fresh:
            out_ref[...] = got
        else:
            out_ref[...] = out_ref[...] + got

    ffn_sets = [uses[a:b] for a, b in zip((0,) + FFN_CUTS, FFN_CUTS + (groups,))]
    ready = []
    for i in range(groups + 1):
        if groups - LAG <= i < groups:
            come_back(i)
        for part in ffn_sets:
            if i > 0 and part[-1] == uses[i - 1]:
                if i == 2:
                    for a in range(3):
                        for k in range(nm - 1):
                            weight_pass(a, k).wait_recv()
                feed_forward(part)
                for g in ready:
                    finish(g, g == uses[0])
                ready = part
    for g in ready:
        finish(g, False)

    for g in range(groups):
        lo = first(g)
        at = pl.ds(lo, per - lo)
        remote(
            spot_out.at[pl.ds(0, per - lo)],
            spot_in.at[g, at],
            s_send.at[g],
            s_recv.at[g],
            mp=others[0],
        ).wait_send()
        remote(
            packed.at[g, at], arr.at[g, at, :, mcols], z_send.at[g], z_recv.at[g], mp=others[0]
        ).wait_send()
        remote(ans.at[g, at], ret.at[g, at], b_send.at[g], b_recv.at[g], mp=others[0]).wait_send()
        for side in range(2):
            share(g, side).wait_send()
            share_on(g, side).wait_send()
        for k in range(nm - 1):
            onward(g, k).wait_send()
            result_copy(g, k).wait_send()
    for i in range(3):
        for side in range(2):
            weight_copy(i, side).wait_send()
            weight_on(i, side).wait_send()
        for k in range(nm - 1):
            weight_pass(i, k).wait_send()


def shards(sizes, *args):
    x, ids, slots, counts, gain, wqk, wv, wo, fgain, wu, wd = args
    nz, nm, ns = sizes
    rows, width = x.shape
    owners = nz * ns
    cap = 2 * rows // owners
    groups = nz // 2
    per = 2 * ns
    grows = per * cap
    vmem = pl.BlockSpec(memory_space=pltpu.VMEM)
    smem = pl.BlockSpec(memory_space=pltpu.SMEM)
    dma = pltpu.SemaphoreType.DMA
    return pl.pallas_call(
        functools.partial(block_kernel, sizes),
        out_shape=jax.ShapeDtypeStruct((rows, LANES), BF16),
        in_specs=[vmem, vmem, vmem, smem] + [vmem] * 7,
        out_specs=vmem,
        scratch_shapes=[
            pltpu.VMEM((rows, LANES), BF16),
            pltpu.VMEM((groups, per, cap, LANES), BF16),
            pltpu.VMEM((owners, 1, LANES), F32),
            pltpu.VMEM((groups, per, 1, LANES), F32),
            pltpu.VMEM((groups, per, cap, width), BF16),
            pltpu.VMEM((groups, grows, LANES), F32),
            pltpu.VMEM((rows, LANES), F32),
            pltpu.VMEM((WIN_DEV * WLEN, 3 * LANES), BF16),
            pltpu.VMEM((LANES, WIN_DEV * WLEN), BF16),
            pltpu.VMEM((groups, per, cap, LANES), BF16),
            pltpu.VMEM((groups, per, cap, LANES), BF16),
            pltpu.VMEM((LANES // HDIM, WLEN, WLEN), F32),
            pltpu.VMEM((LANES // HDIM, WLEN, WLEN), F32),
            pltpu.VMEM((groups, cap, width), BF16),
            pltpu.VMEM((groups, nm, cap, LANES), BF16),
            pltpu.VMEM((groups, nm, cap, LANES), BF16),
            pltpu.VMEM((groups, nm, cap, LANES), BF16),
            dma((groups, 2)),
            dma((groups, 2)),
            pltpu.VMEM((nm,) + wo.shape, BF16),
            pltpu.VMEM((nm,) + wu.shape, BF16),
            pltpu.VMEM((nm,) + wd.shape, BF16),
            dma((groups,)),
            dma((groups,)),
            dma((groups,)),
            dma((groups,)),
            dma((groups, 2)),
            dma((groups, 2)),
            dma((groups,)),
            dma((groups,)),
            dma((3, 2)),
            dma((3, 2)),
            dma((3, 2)),
            dma((3, 2)),
            dma((3, nm - 1)),
            dma((3, nm - 1)),
            dma((groups, nm - 1)),
            dma((groups, nm - 1)),
            dma((groups, nm - 1)),
            dma((groups, nm - 1)),
        ],
        compiler_params=pltpu.CompilerParams(
            collective_id=0, has_side_effects=True, vmem_limit_bytes=60 * 1024 * 1024
        ),
        name="block",
    )(
        x,
        ids,
        slots,
        counts,
        gain.reshape(1, width),
        wqk,
        wv,
        wo,
        fgain.reshape(1, width),
        wu,
        wd,
    )


def solution(mesh):
    sizes = (mesh.shape["space"], mesh.shape["mp"], mesh.shape["sub"])
    return jax.shard_map(
        functools.partial(shards, sizes),
        mesh=mesh,
        in_specs=(
            P(("groups", "space", "sub"), None),
            P(("groups", "space", "sub")),
            P(("groups", "space", "sub")),
            P("groups"),
            P(),
            P(None, None, "mp"),
            P(None, "mp"),
            P("mp", None),
            P(),
            P(None, "mp"),
            P("mp", None),
        ),
        out_specs=P(("groups", "space", "sub"), "mp"),
        check_vma=False,
    )
```

```python
import functools

import jax
import jax.numpy as jnp
from jax import lax
from jax.experimental import pallas as pl
from jax.experimental.pallas import tpu as pltpu
from jax.sharding import PartitionSpec as P

HDIM = 64
CUTS = (1, 2, 3, 4, 5, 6, 7)
AHEAD = 8
BACK = 8
FFN_CUTS = (2, 4, 6, 7)
WLEN = 256
WIN_DEV = 16
LANES = 128
MESH = pl.DeviceIdType.MESH
BF16 = jnp.bfloat16
F32 = jnp.float32


def dot(a, b):
    return jnp.dot(a, b, preferred_element_type=F32)


def dot_nt(a, b):
    return lax.dot_general(a, b, (((1,), (1,)), ((), ())), preferred_element_type=F32)


def dot_tn(a, b):
    return lax.dot_general(a, b, (((0,), (0,)), ((), ())), preferred_element_type=F32)


def pick(mask):
    return jnp.where(mask, 1.0, 0.0).astype(BF16)


def pick16(mask):
    return jnp.where(mask, jnp.ones((), BF16), jnp.zeros((), BF16))


def block_kernel(
    sizes,
    x_ref,
    ids_ref,
    slots_ref,
    counts_ref,
    gain_ref,
    wqk_ref,
    wv_ref,
    wo_ref,
    fgain_ref,
    wu_ref,
    wd_ref,
    out_ref,
    xn,
    packed,
    spot_out,
    spot_in,
    arr,
    spot_col,
    send_col,
    acc,
    mixt,
    ans,
    ret,
    sc_even,
    sc_odd,
    xr,
    hx,
    res,
    rx,
    f_send,
    f_recv,
    wo_all,
    wu_all,
    wd_all,
    z_send,
    z_recv,
    s_send,
    s_recv,
    x_send,
    x_recv,
    b_send,
    b_recv,
    w_send,
    w_recv,
    v_send,
    v_recv,
    d_send,
    d_recv,
    a_send,
    a_recv,
    r_send,
    r_recv,
):
    nz, nm, ns = sizes
    rows, width = x_ref.shape
    owners = nz * ns
    cap = 2 * rows // owners
    groups = nz // 2
    per = 2 * ns
    grows = per * cap
    z = lax.axis_index("space")
    m = lax.axis_index("mp")
    s = lax.axis_index("sub")
    me = z * ns + s
    mcols = pl.ds(pl.multiple_of(m * LANES, LANES), LANES)

    def offset(g, j):
        if g == 0:
            return (0 if j < ns else nz // 2), j % ns
        return (g if j < ns else nz - g), j % ns

    def forward(g, j):
        dz, ds = offset(g, j)
        return lax.rem(z + dz, nz), lax.rem(s + ds, ns)

    def backward(g, j):
        dz, ds = offset(g, j)
        return lax.rem(z + (nz - dz), nz), lax.rem(s + ds, ns)

    def owner(g, j):
        tz, ts = forward(g, j)
        return tz * ns + ts

    def first(g):
        return 1 if g == 0 else 0

    def remote(src, dst, ssem, rsem, **where):
        return pltpu.make_async_remote_copy(
            src_ref=src,
            dst_ref=dst,
            send_sem=ssem,
            recv_sem=rsem,
            device_id=where,
            device_id_type=MESH,
        )

    order = list(range(1, groups)) + [0]
    uses = order
    others = [lax.rem(m + k, nm) for k in range(1, nm)]

    barrier = pltpu.get_barrier_semaphore()
    for g in range(groups):
        for j in range(first(g), per):
            tz, ts = forward(g, j)
            pl.semaphore_signal(
                barrier, inc=1, device_id={"space": tz, "sub": ts}, device_id_type=MESH
            )
    for om in others:
        pl.semaphore_signal(barrier, inc=1, device_id={"mp": om}, device_id_type=MESH)

    def norm_rows(i, carry):
        at = pl.ds(pl.multiple_of(i * 256, 256), 256)
        xb = x_ref[at, :].astype(F32)
        mean = jnp.sum(xb, axis=1, keepdims=True) * (1.0 / width)
        cen = xb - mean
        var = jnp.sum(cen * cen, axis=1, keepdims=True) * (1.0 / width)
        mine = x_ref[at, mcols].astype(F32) - mean
        xn[at, :] = (mine * lax.rsqrt(var + 1e-05) * gain_ref[:, mcols]).astype(BF16)
        return carry

    lax.fori_loop(0, rows // 256, norm_rows, 0)

    ids = ids_ref[...].reshape(1, rows)
    dest = ids // WIN_DEV
    win = ids - dest * WIN_DEV
    owner_iota = lax.broadcasted_iota(jnp.int32, (owners, rows), 0)
    hit = owner_iota == dest
    table = pick(hit)
    step = 256
    earlier = pick(
        lax.broadcasted_iota(jnp.int32, (step, step), 0)
        < lax.broadcasted_iota(jnp.int32, (step, step), 1)
    )
    seen = jnp.zeros((owners, 1), F32)
    ranks = []
    for i in range(rows // step):
        part = table[:, i * step : (i + 1) * step]
        wide = part.astype(F32)
        before = dot(part, earlier) + seen
        ranks.append(jnp.sum(before * wide, axis=0, keepdims=True))
        seen = seen + jnp.sum(wide, axis=1, keepdims=True)
    rank = jnp.concatenate(ranks, axis=1).astype(jnp.int32)
    send = dest * cap + rank
    rank_hit = pick(lax.broadcasted_iota(jnp.int32, (LANES, rows), 0) == rank)
    slot_at = dot_nt(
        jnp.where(hit, (slots_ref[...].reshape(1, rows) + 1).astype(F32), 0.0).astype(BF16), rank_hit
    )
    win_at = dot_nt(jnp.where(hit, win.astype(F32), 0.0).astype(BF16), rank_hit)
    spots = slot_at + win_at * float(WLEN)
    for o in range(owners):
        spot_out[o] = spots[o : o + 1, :]

    pl.semaphore_wait(barrier, groups * per - 1 + nm - 1)

    row_in = lax.broadcasted_iota(jnp.int32, (grows, 1), 0)
    lane_in = lax.broadcasted_iota(jnp.int32, (1, grows), 1)

    def places(g, inner):
        total = inner
        for j in range(per):
            low = owner(g, j) * cap - j * cap
            if j == 0:
                total = inner + low
            else:
                total = jnp.where(inner >= j * cap, inner + low, total)
        return total

    for g in order:
        for j in range(first(g), per):
            tz, ts = forward(g, j)
            remote(
                spot_out.at[owner(g, j)],
                spot_in.at[g, j],
                s_send.at[g],
                s_recv.at[g],
                space=tz,
                sub=ts,
            ).start()

    def pack(g):
        sel = pick(places(g, row_in) == send)
        packed[g] = dot(sel, xn[...]).astype(BF16).reshape(per, cap, LANES)

    def post(i):
        if i < groups:
            g = order[i]
            for j in range(first(g), per):
                tz, ts = forward(g, j)
                remote(
                    packed.at[g, j],
                    arr.at[g, j, :, mcols],
                    z_send.at[g],
                    z_recv.at[g],
                    space=tz,
                    sub=ts,
                ).start()

    for i in range(groups):
        pack(order[i])
        if i < AHEAD:
            post(i)

    mine_iota = lax.broadcasted_iota(jnp.int32, (cap, 1), 0)

    def mine_of(g):
        near, far = (0, nz // 2) if g == 0 else (g, nz - g)
        tz = lax.rem(z + jnp.where(m < ns, near, far), nz)
        ts = lax.rem(s + lax.rem(m, ns), ns)
        return mine_iota + (tz * ns + ts) * cap

    def residual(part):
        at = jnp.concatenate([mine_of(g) for g in part], axis=0)
        got = dot(pick(at == send), x_ref[...]).astype(BF16)
        for n, g in enumerate(part):
            xr[g] = got[n * cap : (n + 1) * cap]

    arr[0, 0, :, mcols] = packed[0, 0]
    spot_in[0, 0] = spot_out[me]
    wo_all[m] = wo_ref[...]
    wu_all[m] = wu_ref[...]
    wd_all[m] = wd_ref[...]
    for i in range(rows // LANES):
        piece = send[:, i * LANES : (i + 1) * LANES].astype(F32)
        send_col[i * LANES : (i + 1) * LANES, :] = jnp.transpose(
            jnp.broadcast_to(piece, (LANES, LANES))
        )

    lane = lax.broadcasted_iota(jnp.int32, (1, LANES), 1)
    wqkv = jnp.concatenate([wqk_ref[0], wqk_ref[1], wv_ref[...]], axis=1)

    def spot_row(g):
        a0, a1, a2, a3 = (spot_in[g, j] for j in range(per))
        r1 = pltpu.roll(a1, 96, 1)
        r2 = pltpu.roll(a2, 64, 1)
        r3 = pltpu.roll(a3, 32, 1)
        t0 = a0 + jnp.where(lane >= 96, r1, 0.0)
        t1 = jnp.where(lane < 64, r1, 0.0) + jnp.where(lane >= 64, r2, 0.0)
        t2 = jnp.where(lane < 32, r2, 0.0) + jnp.where(lane >= 32, r3, 0.0)
        return [t0, t1, t2]

    def gather_wait(g):
        lo = first(g)
        remote(
            spot_out.at[pl.ds(0, per - lo)],
            spot_in.at[g, pl.ds(lo, per - lo)],
            s_send.at[g],
            s_recv.at[g],
            mp=others[0],
        ).wait_recv()
        remote(
            packed.at[g, pl.ds(lo, per - lo)],
            arr.at[g, pl.ds(lo, per - lo), :, mcols],
            z_send.at[g],
            z_recv.at[g],
            mp=others[0],
        ).wait_recv()

    sides = (lax.rem(m + 1, nm), lax.rem(m + nm - 1, nm))

    def cols(who):
        return pl.ds(pl.multiple_of(who * LANES, LANES), LANES)

    def share(g, side):
        ref = arr.at[g, :, :, mcols]
        return remote(ref, ref, x_send.at[g, side], x_recv.at[g, side], mp=sides[side])

    def share_on(g, side):
        half = pl.ds(side * (per // 2), per // 2)
        ref = arr.at[g, half, :, cols(sides[1 - side])]
        return remote(ref, ref, f_send.at[g, side], f_recv.at[g, side], mp=sides[side])

    def regroup(pair, fresh):
        parts = []
        for g in pair:
            tiles = spot_row(g)
            parts += tiles
            for i, t in enumerate(tiles):
                spot_col[g, i * LANES : (i + 1) * LANES, :] = jnp.transpose(
                    jnp.broadcast_to(t, (LANES, LANES))
                )
        row = jnp.concatenate(parts, axis=1).astype(jnp.int32) - 1
        row_win = row // WLEN
        row_slot = (row - row_win * WLEN).astype(F32)
        held = jnp.concatenate([arr[g].reshape(grows, width) for g in pair], axis=0)
        proj = dot(held, wqkv).astype(BF16)
        slot_iota = lax.broadcasted_iota(jnp.int32, (WLEN, row.shape[1]), 0).astype(F32).astype(BF16)
        few = 4

        def some_windows(i, carry):
            sels = []
            for n in range(few):
                key = jnp.where(row_win == i * few + n, row_slot, -1.0).astype(BF16)
                sels.append(pick16(slot_iota == key))
            got = dot(jnp.concatenate(sels, axis=0), proj).astype(BF16)
            at = pl.ds(pl.multiple_of(i * (few * WLEN), few * WLEN), few * WLEN)
            if fresh:
                acc[at, :] = got
            else:
                acc[at, :] = acc[at, :] + got
            return carry

        lax.fori_loop(0, WIN_DEV // few, some_windows, 0)

    sets = [uses[a:b] for a, b in zip((0,) + CUTS, CUTS + (groups,))]

    def stage(i):
        if 0 <= i < groups:
            gather_wait(uses[i])
            post(i + AHEAD)
            for side in range(2):
                share(uses[i], side).start()

    def stage_on(i):
        if 0 <= i < groups:
            for side in range(2):
                share(uses[i], side).wait_recv()
                share_on(uses[i], side).start()

    def stage_use(i):
        for n, part in enumerate(sets):
            if 0 <= i < groups and part[-1] == uses[i]:
                for g in part:
                    for side in range(2):
                        share_on(g, side).wait_recv()
                regroup(part, n == 0)

    for i in range(groups):
        stage(i)
        stage_use(i - 1)
        stage_on(i)
        if i in (2, 4):
            residual(uses[:groups // 2] if i == 2 else uses[groups // 2:])
    kept = ((wu_ref, wu_all), (wd_ref, wd_all), (wo_ref, wo_all))

    def weight_copy(i, side):
        ref, all_ref = kept[i]
        half = ref.shape[0] // ns
        at = pl.ds(pl.multiple_of(s * half, half), half)
        return remote(
            ref.at[at], all_ref.at[m, at], w_send.at[i, side], w_recv.at[i, side], mp=sides[side]
        )

    def weight_on(i, side):
        ref, all_ref = kept[i]
        half = ref.shape[0] // ns
        low = half // 2
        at = pl.ds(pl.multiple_of(s * half + side * low, low), low)
        part = all_ref.at[sides[1 - side], at]
        return remote(part, part, v_send.at[i, side], v_recv.at[i, side], mp=sides[side])

    def weight_pass(i, k):
        ref, all_ref = kept[i]
        half = ref.shape[0] // ns
        at = pl.ds(pl.multiple_of(s * half, half), half)
        part = all_ref.at[others[k], at]
        return remote(part, part, d_send.at[i, k], d_recv.at[i, k], sub=lax.rem(s + 1, ns))

    def weights_on(side):
        for i in range(3):
            weight_copy(i, side).wait_recv()
            weight_on(i, side).start()

    for i in range(3):
        for side in range(2):
            weight_copy(i, side).start()

    stage_use(groups - 1)

    key_iota = lax.broadcasted_iota(jnp.int32, (WLEN, LANES), 0)
    heads_here = LANES // HDIM
    head_of = lane // HDIM
    own = [jnp.where(head_of == h, 1.0, 0.0).astype(BF16) for h in range(heads_here)]
    extra = [jnp.where(lane == (heads_here - 1 - h) * HDIM, 1.0, 0.0) for h in range(heads_here)]
    ones = jnp.ones((16, WLEN), BF16)

    def score(w, sc_ref):
        here = acc[pl.ds(pl.multiple_of(w * WLEN, WLEN), WLEN), :]
        q = here[:, :LANES] * jnp.asarray(HDIM**-0.5, BF16)
        k = here[:, LANES : 2 * LANES]
        dead = jnp.where(key_iota < counts_ref[me * WIN_DEV + w], 0.0, -1e30)
        for h in range(heads_here):
            qh = q * own[h] + extra[h].astype(BF16)
            kh = k * own[h] + (dead * extra[h]).astype(BF16)
            sc_ref[h] = dot_nt(kh, qh)

    def mix(w, sc_ref):
        at = pl.ds(pl.multiple_of(w * WLEN, WLEN), WLEN)
        vt = jnp.transpose(acc[at, 2 * LANES :].astype(F32)).astype(BF16)
        parts = []
        for h in range(heads_here):
            sc = sc_ref[h]
            weights = jnp.exp(sc - jnp.max(sc, axis=0, keepdims=True)).astype(BF16)
            both = jnp.concatenate([vt[h * HDIM : (h + 1) * HDIM], ones], axis=0)
            got = dot(both, weights)
            parts.append(got[:HDIM] / got[HDIM : HDIM + 1])
        mixt[:, at] = jnp.concatenate(parts, axis=0).astype(BF16)

    def attend(i, carry):
        score(2 * i + 1, sc_odd)
        mix(2 * i, sc_even)
        score(jnp.minimum(2 * i + 2, WIN_DEV - 1), sc_even)
        mix(2 * i + 1, sc_odd)
        return carry

    score(0, sc_even)
    lax.fori_loop(0, WIN_DEV // 2, attend, 0)

    span = 4 * WLEN
    span_iota = lax.broadcasted_iota(jnp.int32, (1, span), 1)

    def answer(i):
        if i < groups:
            g = order[i]
            for j in range(first(g), per):
                tz, ts = backward(g, j)
                remote(
                    ans.at[g, j], ret.at[g, j], b_send.at[g], b_recv.at[g], space=tz, sub=ts
                ).start()

    for n, g in enumerate(order):
        col = spot_col[g].astype(jnp.int32)
        wide = jnp.concatenate([col] * (span // LANES), axis=1)

        def gather(c, total):
            at = pl.ds(pl.multiple_of(c * span, span), span)
            return total + dot_nt(pick(wide == span_iota + (c * span + 1)), mixt[:, at])

        total = lax.fori_loop(
            0, WIN_DEV * WLEN // span, gather, jnp.zeros((grows, LANES), F32)
        )
        ans[g] = total.astype(BF16).reshape(per, cap, LANES)
        if n < BACK:
            answer(n)
        if n == groups // 2:
            for side in range(2):
                weights_on(side)
    ret[0, 0] = ans[0, 0]

    def onward(g, k):
        return remote(
            ret.at[g, others[k]], hx.at[g, m], a_send.at[g, k], a_recv.at[g, k], mp=others[k]
        )

    def result_copy(g, k):
        return remote(
            res.at[g, others[k]], rx.at[g, m], r_send.at[g, k], r_recv.at[g, k], mp=others[k]
        )

    def come_back(i):
        g = uses[i]
        at = pl.ds(first(g), per - first(g))
        remote(
            ans.at[g, at], ret.at[g, at], b_send.at[g], b_recv.at[g], mp=others[0]
        ).wait_recv()
        answer(i + BACK)
        for k in range(nm - 1):
            onward(g, k).start()
        hx[g, m] = ret[g, m]

    def feed_forward(part):
        for g in part:
            for k in range(nm - 1):
                onward(g, k).wait_recv()
        heads = jnp.concatenate(
            [jnp.concatenate([hx[g, k] for k in range(nm)], axis=1) for g in part], axis=0
        )
        stream = jnp.concatenate([xr[g] for g in part], axis=0).astype(F32)
        after = stream + dot(heads, wo_all[...].reshape(width, width))
        mean = jnp.sum(after, axis=1, keepdims=True) * (1.0 / width)
        cen = after - mean
        var = jnp.sum(cen * cen, axis=1, keepdims=True) * (1.0 / width)
        normed = (cen * lax.rsqrt(var + 1e-05) * fgain_ref[...]).astype(BF16)
        total = after
        for c in range(nm):
            up = dot(normed, wu_all[c])
            inner = 0.7978845608028654 * (up + 0.044715 * (up * up * up))
            hidden = (0.5 * up * (1.0 + jnp.tanh(inner))).astype(BF16)
            total = total + dot(hidden, wd_all[c])
        total = total.astype(BF16)
        for n, g in enumerate(part):
            for k in range(nm):
                res[g, k] = total[n * cap : (n + 1) * cap, k * LANES : (k + 1) * LANES]
            for k in range(nm - 1):
                result_copy(g, k).start()
            rx[g, m] = res[g, m]

    wide_send = send_col[...].astype(jnp.int32)
    wide_send = jnp.concatenate([wide_send] * (grows // LANES), axis=1)

    def finish(g, fresh):
        for k in range(nm - 1):
            result_copy(g, k).wait_recv()
        got = dot(
            pick(wide_send == places(g, lane_in)), rx[g].reshape(grows, LANES)
        ).astype(BF16)
        if fresh:
            out_ref[...] = got
        else:
            out_ref[...] = out_ref[...] + got

    ffn_sets = [uses[a:b] for a, b in zip((0,) + FFN_CUTS, FFN_CUTS + (groups,))]
    ready = []
    for i in range(groups + 1):
        if i < groups:
            come_back(i)
        if i == 1:
            for a in range(3):
                for side in range(2):
                    weight_on(a, side).wait_recv()
                for k in range(nm - 1):
                    weight_pass(a, k).start()
        for part in ffn_sets:
            if i > 0 and part[-1] == uses[i - 1]:
                if i == 2:
                    for a in range(3):
                        for k in range(nm - 1):
                            weight_pass(a, k).wait_recv()
                feed_forward(part)
                for g in ready:
                    finish(g, g == uses[0])
                ready = part
    for g in ready:
        finish(g, False)

    for g in range(groups):
        lo = first(g)
        at = pl.ds(lo, per - lo)
        remote(
            spot_out.at[pl.ds(0, per - lo)],
            spot_in.at[g, at],
            s_send.at[g],
            s_recv.at[g],
            mp=others[0],
        ).wait_send()
        remote(
            packed.at[g, at], arr.at[g, at, :, mcols], z_send.at[g], z_recv.at[g], mp=others[0]
        ).wait_send()
        remote(ans.at[g, at], ret.at[g, at], b_send.at[g], b_recv.at[g], mp=others[0]).wait_send()
        for side in range(2):
            share(g, side).wait_send()
            share_on(g, side).wait_send()
        for k in range(nm - 1):
            onward(g, k).wait_send()
            result_copy(g, k).wait_send()
    for i in range(3):
        for side in range(2):
            weight_copy(i, side).wait_send()
            weight_on(i, side).wait_send()
        for k in range(nm - 1):
            weight_pass(i, k).wait_send()


def shards(sizes, *args):
    x, ids, slots, counts, gain, wqk, wv, wo, fgain, wu, wd = args
    nz, nm, ns = sizes
    rows, width = x.shape
    owners = nz * ns
    cap = 2 * rows // owners
    groups = nz // 2
    per = 2 * ns
    grows = per * cap
    vmem = pl.BlockSpec(memory_space=pltpu.VMEM)
    smem = pl.BlockSpec(memory_space=pltpu.SMEM)
    dma = pltpu.SemaphoreType.DMA
    return pl.pallas_call(
        functools.partial(block_kernel, sizes),
        out_shape=jax.ShapeDtypeStruct((rows, LANES), BF16),
        in_specs=[vmem, vmem, vmem, smem] + [vmem] * 7,
        out_specs=vmem,
        scratch_shapes=[
            pltpu.VMEM((rows, LANES), BF16),
            pltpu.VMEM((groups, per, cap, LANES), BF16),
            pltpu.VMEM((owners, 1, LANES), F32),
            pltpu.VMEM((groups, per, 1, LANES), F32),
            pltpu.VMEM((groups, per, cap, width), BF16),
            pltpu.VMEM((groups, grows, LANES), F32),
            pltpu.VMEM((rows, LANES), F32),
            pltpu.VMEM((WIN_DEV * WLEN, 3 * LANES), BF16),
            pltpu.VMEM((LANES, WIN_DEV * WLEN), BF16),
            pltpu.VMEM((groups, per, cap, LANES), BF16),
            pltpu.VMEM((groups, per, cap, LANES), BF16),
            pltpu.VMEM((LANES // HDIM, WLEN, WLEN), F32),
            pltpu.VMEM((LANES // HDIM, WLEN, WLEN), F32),
            pltpu.VMEM((groups, cap, width), BF16),
            pltpu.VMEM((groups, nm, cap, LANES), BF16),
            pltpu.VMEM((groups, nm, cap, LANES), BF16),
            pltpu.VMEM((groups, nm, cap, LANES), BF16),
            dma((groups, 2)),
            dma((groups, 2)),
            pltpu.VMEM((nm,) + wo.shape, BF16),
            pltpu.VMEM((nm,) + wu.shape, BF16),
            pltpu.VMEM((nm,) + wd.shape, BF16),
            dma((groups,)),
            dma((groups,)),
            dma((groups,)),
            dma((groups,)),
            dma((groups, 2)),
            dma((groups, 2)),
            dma((groups,)),
            dma((groups,)),
            dma((3, 2)),
            dma((3, 2)),
            dma((3, 2)),
            dma((3, 2)),
            dma((3, nm - 1)),
            dma((3, nm - 1)),
            dma((groups, nm - 1)),
            dma((groups, nm - 1)),
            dma((groups, nm - 1)),
            dma((groups, nm - 1)),
        ],
        compiler_params=pltpu.CompilerParams(
            collective_id=0, has_side_effects=True, vmem_limit_bytes=60 * 1024 * 1024
        ),
        name="block",
    )(
        x,
        ids,
        slots,
        counts,
        gain.reshape(1, width),
        wqk,
        wv,
        wo,
        fgain.reshape(1, width),
        wu,
        wd,
    )


def solution(mesh):
    sizes = (mesh.shape["space"], mesh.shape["mp"], mesh.shape["sub"])
    return jax.shard_map(
        functools.partial(shards, sizes),
        mesh=mesh,
        in_specs=(
            P(("groups", "space", "sub"), None),
            P(("groups", "space", "sub")),
            P(("groups", "space", "sub")),
            P("groups"),
            P(),
            P(None, None, "mp"),
            P(None, "mp"),
            P("mp", None),
            P(),
            P(None, "mp"),
            P("mp", None),
        ),
        out_specs=P(("groups", "space", "sub"), "mp"),
        check_vma=False,
    )
```

```python
import functools

import jax
import jax.numpy as jnp
from jax import lax
from jax.experimental import pallas as pl
from jax.experimental.pallas import tpu as pltpu
from jax.sharding import PartitionSpec as P

HDIM = 64
CUTS = (1, 2, 3, 4, 5, 6, 7)
AHEAD = 8
BACK = 8
FFN_CUTS = (2, 4, 6, 7)
WLEN = 256
WIN_DEV = 16
LANES = 128
MESH = pl.DeviceIdType.MESH
BF16 = jnp.bfloat16
F32 = jnp.float32


def dot(a, b):
    return jnp.dot(a, b, preferred_element_type=F32)


def dot_nt(a, b):
    return lax.dot_general(a, b, (((1,), (1,)), ((), ())), preferred_element_type=F32)


def dot_tn(a, b):
    return lax.dot_general(a, b, (((0,), (0,)), ((), ())), preferred_element_type=F32)


def pick(mask):
    return jnp.where(mask, 1.0, 0.0).astype(BF16)


def pick16(mask):
    return jnp.where(mask, jnp.ones((), BF16), jnp.zeros((), BF16))


def block_kernel(
    sizes,
    x_ref,
    ids_ref,
    slots_ref,
    counts_ref,
    gain_ref,
    wqk_ref,
    wv_ref,
    wo_ref,
    fgain_ref,
    wu_ref,
    wd_ref,
    out_ref,
    xn,
    packed,
    spot_out,
    spot_in,
    arr,
    spot_col,
    send_col,
    acc,
    mixt,
    ans,
    ret,
    sc_even,
    sc_odd,
    xr,
    hx,
    res,
    rx,
    f_send,
    f_recv,
    wo_all,
    wu_all,
    wd_all,
    z_send,
    z_recv,
    s_send,
    s_recv,
    x_send,
    x_recv,
    b_send,
    b_recv,
    w_send,
    w_recv,
    v_send,
    v_recv,
    d_send,
    d_recv,
    a_send,
    a_recv,
    r_send,
    r_recv,
):
    nz, nm, ns = sizes
    rows, width = x_ref.shape
    owners = nz * ns
    cap = 2 * rows // owners
    groups = nz // 2
    per = 2 * ns
    grows = per * cap
    z = lax.axis_index("space")
    m = lax.axis_index("mp")
    s = lax.axis_index("sub")
    me = z * ns + s
    mcols = pl.ds(pl.multiple_of(m * LANES, LANES), LANES)

    def offset(g, j):
        if g == 0:
            return (0 if j < ns else nz // 2), j % ns
        return (g if j < ns else nz - g), j % ns

    def forward(g, j):
        dz, ds = offset(g, j)
        return lax.rem(z + dz, nz), lax.rem(s + ds, ns)

    def backward(g, j):
        dz, ds = offset(g, j)
        return lax.rem(z + (nz - dz), nz), lax.rem(s + ds, ns)

    def owner(g, j):
        tz, ts = forward(g, j)
        return tz * ns + ts

    def first(g):
        return 1 if g == 0 else 0

    def remote(src, dst, ssem, rsem, **where):
        return pltpu.make_async_remote_copy(
            src_ref=src,
            dst_ref=dst,
            send_sem=ssem,
            recv_sem=rsem,
            device_id=where,
            device_id_type=MESH,
        )

    order = list(range(1, groups)) + [0]
    uses = order
    others = [lax.rem(m + k, nm) for k in range(1, nm)]

    barrier = pltpu.get_barrier_semaphore()
    for g in range(groups):
        for j in range(first(g), per):
            tz, ts = forward(g, j)
            pl.semaphore_signal(
                barrier, inc=1, device_id={"space": tz, "sub": ts}, device_id_type=MESH
            )
    for om in others:
        pl.semaphore_signal(barrier, inc=1, device_id={"mp": om}, device_id_type=MESH)

    def norm_rows(i, carry):
        at = pl.ds(pl.multiple_of(i * 256, 256), 256)
        xb = x_ref[at, :].astype(F32)
        mean = jnp.sum(xb, axis=1, keepdims=True) * (1.0 / width)
        cen = xb - mean
        var = jnp.sum(cen * cen, axis=1, keepdims=True) * (1.0 / width)
        mine = x_ref[at, mcols].astype(F32) - mean
        xn[at, :] = (mine * lax.rsqrt(var + 1e-05) * gain_ref[:, mcols]).astype(BF16)
        return carry

    lax.fori_loop(0, rows // 256, norm_rows, 0)

    ids = ids_ref[...].reshape(1, rows)
    dest = ids // WIN_DEV
    win = ids - dest * WIN_DEV
    owner_iota = lax.broadcasted_iota(jnp.int32, (owners, rows), 0)
    hit = owner_iota == dest
    table = pick(hit)
    step = 256
    earlier = pick(
        lax.broadcasted_iota(jnp.int32, (step, step), 0)
        < lax.broadcasted_iota(jnp.int32, (step, step), 1)
    )
    seen = jnp.zeros((owners, 1), F32)
    ranks = []
    for i in range(rows // step):
        part = table[:, i * step : (i + 1) * step]
        wide = part.astype(F32)
        before = dot(part, earlier) + seen
        ranks.append(jnp.sum(before * wide, axis=0, keepdims=True))
        seen = seen + jnp.sum(wide, axis=1, keepdims=True)
    rank = jnp.concatenate(ranks, axis=1).astype(jnp.int32)
    send = dest * cap + rank
    rank_hit = pick(lax.broadcasted_iota(jnp.int32, (LANES, rows), 0) == rank)
    slot_at = dot_nt(
        jnp.where(hit, (slots_ref[...].reshape(1, rows) + 1).astype(F32), 0.0).astype(BF16), rank_hit
    )
    win_at = dot_nt(jnp.where(hit, win.astype(F32), 0.0).astype(BF16), rank_hit)
    spots = slot_at + win_at * float(WLEN)
    for o in range(owners):
        spot_out[o] = spots[o : o + 1, :]

    pl.semaphore_wait(barrier, groups * per - 1 + nm - 1)

    row_in = lax.broadcasted_iota(jnp.int32, (grows, 1), 0)
    lane_in = lax.broadcasted_iota(jnp.int32, (1, grows), 1)

    def places(g, inner):
        total = inner
        for j in range(per):
            low = owner(g, j) * cap - j * cap
            if j == 0:
                total = inner + low
            else:
                total = jnp.where(inner >= j * cap, inner + low, total)
        return total

    for g in order:
        for j in range(first(g), per):
            tz, ts = forward(g, j)
            remote(
                spot_out.at[owner(g, j)],
                spot_in.at[g, j],
                s_send.at[g],
                s_recv.at[g],
                space=tz,
                sub=ts,
            ).start()

    def pack(g):
        sel = pick(places(g, row_in) == send)
        packed[g] = dot(sel, xn[...]).astype(BF16).reshape(per, cap, LANES)

    def post(i):
        if i < groups:
            g = order[i]
            for j in range(first(g), per):
                tz, ts = forward(g, j)
                remote(
                    packed.at[g, j],
                    arr.at[g, j, :, mcols],
                    z_send.at[g],
                    z_recv.at[g],
                    space=tz,
                    sub=ts,
                ).start()

    for i in range(groups):
        pack(order[i])
        if i < AHEAD:
            post(i)

    mine_iota = lax.broadcasted_iota(jnp.int32, (cap, 1), 0)

    def mine_of(g):
        near, far = (0, nz // 2) if g == 0 else (g, nz - g)
        tz = lax.rem(z + jnp.where(m < ns, near, far), nz)
        ts = lax.rem(s + lax.rem(m, ns), ns)
        return mine_iota + (tz * ns + ts) * cap

    def residual(part):
        at = jnp.concatenate([mine_of(g) for g in part], axis=0)
        got = dot(pick(at == send), x_ref[...]).astype(BF16)
        for n, g in enumerate(part):
            xr[g] = got[n * cap : (n + 1) * cap]

    arr[0, 0, :, mcols] = packed[0, 0]
    spot_in[0, 0] = spot_out[me]
    wo_all[m] = wo_ref[...]
    wu_all[m] = wu_ref[...]
    wd_all[m] = wd_ref[...]
    for i in range(rows // LANES):
        piece = send[:, i * LANES : (i + 1) * LANES].astype(F32)
        send_col[i * LANES : (i + 1) * LANES, :] = jnp.transpose(
            jnp.broadcast_to(piece, (LANES, LANES))
        )

    lane = lax.broadcasted_iota(jnp.int32, (1, LANES), 1)
    wqkv = jnp.concatenate([wqk_ref[0], wqk_ref[1], wv_ref[...]], axis=1)

    def spot_row(g):
        a0, a1, a2, a3 = (spot_in[g, j] for j in range(per))
        r1 = pltpu.roll(a1, 96, 1)
        r2 = pltpu.roll(a2, 64, 1)
        r3 = pltpu.roll(a3, 32, 1)
        t0 = a0 + jnp.where(lane >= 96, r1, 0.0)
        t1 = jnp.where(lane < 64, r1, 0.0) + jnp.where(lane >= 64, r2, 0.0)
        t2 = jnp.where(lane < 32, r2, 0.0) + jnp.where(lane >= 32, r3, 0.0)
        return [t0, t1, t2]

    def gather_wait(g):
        lo = first(g)
        remote(
            spot_out.at[pl.ds(0, per - lo)],
            spot_in.at[g, pl.ds(lo, per - lo)],
            s_send.at[g],
            s_recv.at[g],
            mp=others[0],
        ).wait_recv()
        remote(
            packed.at[g, pl.ds(lo, per - lo)],
            arr.at[g, pl.ds(lo, per - lo), :, mcols],
            z_send.at[g],
            z_recv.at[g],
            mp=others[0],
        ).wait_recv()

    sides = (lax.rem(m + 1, nm), lax.rem(m + nm - 1, nm))

    def cols(who):
        return pl.ds(pl.multiple_of(who * LANES, LANES), LANES)

    def share(g, side):
        ref = arr.at[g, :, :, mcols]
        return remote(ref, ref, x_send.at[g, side], x_recv.at[g, side], mp=sides[side])

    def share_on(g, side):
        half = pl.ds(side * (per // 2), per // 2)
        ref = arr.at[g, half, :, cols(sides[1 - side])]
        return remote(ref, ref, f_send.at[g, side], f_recv.at[g, side], mp=sides[side])

    def regroup(pair, fresh):
        parts = []
        for g in pair:
            tiles = spot_row(g)
            parts += tiles
            for i, t in enumerate(tiles):
                spot_col[g, i * LANES : (i + 1) * LANES, :] = jnp.transpose(
                    jnp.broadcast_to(t, (LANES, LANES))
                )
        row = jnp.concatenate(parts, axis=1).astype(jnp.int32) - 1
        row_win = row // WLEN
        row_slot = (row - row_win * WLEN).astype(F32)
        held = jnp.concatenate([arr[g].reshape(grows, width) for g in pair], axis=0)
        proj = dot(held, wqkv).astype(BF16)
        slot_iota = lax.broadcasted_iota(jnp.int32, (WLEN, row.shape[1]), 0).astype(F32).astype(BF16)
        few = 4

        def some_windows(i, carry):
            sels = []
            for n in range(few):
                key = jnp.where(row_win == i * few + n, row_slot, -1.0).astype(BF16)
                sels.append(pick16(slot_iota == key))
            got = dot(jnp.concatenate(sels, axis=0), proj).astype(BF16)
            at = pl.ds(pl.multiple_of(i * (few * WLEN), few * WLEN), few * WLEN)
            if fresh:
                acc[at, :] = got
            else:
                acc[at, :] = acc[at, :] + got
            return carry

        lax.fori_loop(0, WIN_DEV // few, some_windows, 0)

    sets = [uses[a:b] for a, b in zip((0,) + CUTS, CUTS + (groups,))]

    def stage(i):
        if 0 <= i < groups:
            gather_wait(uses[i])
            post(i + AHEAD)
            for side in range(2):
                share(uses[i], side).start()

    def stage_on(i):
        if 0 <= i < groups:
            for side in range(2):
                share(uses[i], side).wait_recv()
                share_on(uses[i], side).start()

    def stage_use(i):
        for n, part in enumerate(sets):
            if 0 <= i < groups and part[-1] == uses[i]:
                for g in part:
                    for side in range(2):
                        share_on(g, side).wait_recv()
                regroup(part, n == 0)

    for i in range(groups):
        stage(i)
        stage_use(i - 1)
        stage_on(i)
        if i in (2, 4):
            residual(uses[:groups // 2] if i == 2 else uses[groups // 2:])
    kept = ((wu_ref, wu_all), (wd_ref, wd_all), (wo_ref, wo_all))

    def weight_copy(i, side):
        ref, all_ref = kept[i]
        half = ref.shape[0] // ns
        at = pl.ds(pl.multiple_of(s * half, half), half)
        return remote(
            ref.at[at], all_ref.at[m, at], w_send.at[i, side], w_recv.at[i, side], mp=sides[side]
        )

    def weight_on(i, side):
        ref, all_ref = kept[i]
        half = ref.shape[0] // ns
        low = half // 2
        at = pl.ds(pl.multiple_of(s * half + side * low, low), low)
        part = all_ref.at[sides[1 - side], at]
        return remote(part, part, v_send.at[i, side], v_recv.at[i, side], mp=sides[side])

    def weight_pass(i, k):
        ref, all_ref = kept[i]
        half = ref.shape[0] // ns
        at = pl.ds(pl.multiple_of(s * half, half), half)
        part = all_ref.at[others[k], at]
        return remote(part, part, d_send.at[i, k], d_recv.at[i, k], sub=lax.rem(s + 1, ns))

    def weights_on(side):
        for i in range(3):
            weight_copy(i, side).wait_recv()
            weight_on(i, side).start()

    for i in range(3):
        for side in range(2):
            weight_copy(i, side).start()

    stage_use(groups - 1)

    key_iota = lax.broadcasted_iota(jnp.int32, (WLEN, LANES), 0)
    heads_here = LANES // HDIM
    head_of = lane // HDIM
    own = [jnp.where(head_of == h, 1.0, 0.0).astype(BF16) for h in range(heads_here)]
    extra = [jnp.where(lane == (heads_here - 1 - h) * HDIM, 1.0, 0.0) for h in range(heads_here)]
    ones = jnp.ones((16, WLEN), BF16)

    def score(w, sc_ref):
        here = acc[pl.ds(pl.multiple_of(w * WLEN, WLEN), WLEN), :]
        q = here[:, :LANES] * jnp.asarray(HDIM**-0.5, BF16)
        k = here[:, LANES : 2 * LANES]
        dead = jnp.where(key_iota < counts_ref[me * WIN_DEV + w], 0.0, -1e30)
        for h in range(heads_here):
            qh = q * own[h] + extra[h].astype(BF16)
            kh = k * own[h] + (dead * extra[h]).astype(BF16)
            sc_ref[h] = dot_nt(kh, qh)

    def mix(w, sc_ref):
        at = pl.ds(pl.multiple_of(w * WLEN, WLEN), WLEN)
        vt = jnp.transpose(acc[at, 2 * LANES :].astype(F32)).astype(BF16)
        parts = []
        for h in range(heads_here):
            sc = sc_ref[h]
            weights = jnp.exp(sc - jnp.max(sc, axis=0, keepdims=True)).astype(BF16)
            both = jnp.concatenate([vt[h * HDIM : (h + 1) * HDIM], ones], axis=0)
            got = dot(both, weights)
            parts.append(got[:HDIM] / got[HDIM : HDIM + 1])
        mixt[:, at] = jnp.concatenate(parts, axis=0).astype(BF16)

    def attend(i, carry):
        score(2 * i + 1, sc_odd)
        mix(2 * i, sc_even)
        score(jnp.minimum(2 * i + 2, WIN_DEV - 1), sc_even)
        mix(2 * i + 1, sc_odd)
        return carry

    score(0, sc_even)
    lax.fori_loop(0, WIN_DEV // 2, attend, 0)

    span = 4 * WLEN
    lane_iota = lax.broadcasted_iota(jnp.int32, (grows, LANES), 1)
    lane_tiles = [(lane_iota + i).astype(F32).astype(BF16) for i in range(0, WLEN, LANES)]

    def answer(i):
        if i < groups:
            g = order[i]
            for j in range(first(g), per):
                tz, ts = backward(g, j)
                remote(
                    ans.at[g, j], ret.at[g, j], b_send.at[g], b_recv.at[g], space=tz, sub=ts
                ).start()

    for n, g in enumerate(order):
        col = spot_col[g].astype(jnp.int32) - 1
        col_win = col // WLEN
        col_slot = (col - col_win * WLEN).astype(F32)

        def gather(c, total):
            at = pl.ds(pl.multiple_of(c * span, span), span)
            tiles = []
            for n in range(span // WLEN):
                key = jnp.where(col_win == c * (span // WLEN) + n, col_slot, -1.0).astype(BF16)
                tiles += [pick16(key == tile) for tile in lane_tiles]
            return total + dot_nt(jnp.concatenate(tiles, axis=1), mixt[:, at])

        total = lax.fori_loop(
            0, WIN_DEV * WLEN // span, gather, jnp.zeros((grows, LANES), F32)
        )
        ans[g] = total.astype(BF16).reshape(per, cap, LANES)
        if n < BACK:
            answer(n)
        if n == 0:
            for side in range(2):
                weights_on(side)
    ret[0, 0] = ans[0, 0]

    for i in range(3):
        for side in range(2):
            weight_on(i, side).wait_recv()
        for k in range(nm - 1):
            weight_pass(i, k).start()

    def onward(g, k):
        return remote(
            ret.at[g, others[k]], hx.at[g, m], a_send.at[g, k], a_recv.at[g, k], mp=others[k]
        )

    def result_copy(g, k):
        return remote(
            res.at[g, others[k]], rx.at[g, m], r_send.at[g, k], r_recv.at[g, k], mp=others[k]
        )

    def come_back(i):
        g = uses[i]
        at = pl.ds(first(g), per - first(g))
        remote(
            ans.at[g, at], ret.at[g, at], b_send.at[g], b_recv.at[g], mp=others[0]
        ).wait_recv()
        answer(i + BACK)
        for k in range(nm - 1):
            onward(g, k).start()
        hx[g, m] = ret[g, m]

    def feed_forward(part):
        for g in part:
            for k in range(nm - 1):
                onward(g, k).wait_recv()
        heads = jnp.concatenate(
            [jnp.concatenate([hx[g, k] for k in range(nm)], axis=1) for g in part], axis=0
        )
        stream = jnp.concatenate([xr[g] for g in part], axis=0).astype(F32)
        after = stream + dot(heads, wo_all[...].reshape(width, width))
        mean = jnp.sum(after, axis=1, keepdims=True) * (1.0 / width)
        cen = after - mean
        var = jnp.sum(cen * cen, axis=1, keepdims=True) * (1.0 / width)
        normed = (cen * lax.rsqrt(var + 1e-05) * fgain_ref[...]).astype(BF16)
        total = after
        for c in range(nm):
            up = dot(normed, wu_all[c])
            inner = 0.7978845608028654 * (up + 0.044715 * (up * up * up))
            hidden = (0.5 * up * (1.0 + jnp.tanh(inner))).astype(BF16)
            total = total + dot(hidden, wd_all[c])
        total = total.astype(BF16)
        for n, g in enumerate(part):
            for k in range(nm):
                res[g, k] = total[n * cap : (n + 1) * cap, k * LANES : (k + 1) * LANES]
            for k in range(nm - 1):
                result_copy(g, k).start()
            rx[g, m] = res[g, m]

    wide_send = send_col[...].astype(jnp.int32)
    wide_send = jnp.concatenate([wide_send] * (grows // LANES), axis=1)

    def finish(g, fresh):
        for k in range(nm - 1):
            result_copy(g, k).wait_recv()
        got = dot(
            pick(wide_send == places(g, lane_in)), rx[g].reshape(grows, LANES)
        ).astype(BF16)
        if fresh:
            out_ref[...] = got
        else:
            out_ref[...] = out_ref[...] + got

    ffn_sets = [uses[a:b] for a, b in zip((0,) + FFN_CUTS, FFN_CUTS + (groups,))]
    ready = []
    for i in range(groups + 1):
        if i < groups:
            come_back(i)
        for part in ffn_sets:
            if i > 0 and part[-1] == uses[i - 1]:
                if i == 2:
                    for a in range(3):
                        for k in range(nm - 1):
                            weight_pass(a, k).wait_recv()
                feed_forward(part)
                for g in ready:
                    finish(g, g == uses[0])
                ready = part
    for g in ready:
        finish(g, False)

    for g in range(groups):
        lo = first(g)
        at = pl.ds(lo, per - lo)
        remote(
            spot_out.at[pl.ds(0, per - lo)],
            spot_in.at[g, at],
            s_send.at[g],
            s_recv.at[g],
            mp=others[0],
        ).wait_send()
        remote(
            packed.at[g, at], arr.at[g, at, :, mcols], z_send.at[g], z_recv.at[g], mp=others[0]
        ).wait_send()
        remote(ans.at[g, at], ret.at[g, at], b_send.at[g], b_recv.at[g], mp=others[0]).wait_send()
        for side in range(2):
            share(g, side).wait_send()
            share_on(g, side).wait_send()
        for k in range(nm - 1):
            onward(g, k).wait_send()
            result_copy(g, k).wait_send()
    for i in range(3):
        for side in range(2):
            weight_copy(i, side).wait_send()
            weight_on(i, side).wait_send()
        for k in range(nm - 1):
            weight_pass(i, k).wait_send()


def shards(sizes, *args):
    x, ids, slots, counts, gain, wqk, wv, wo, fgain, wu, wd = args
    nz, nm, ns = sizes
    rows, width = x.shape
    owners = nz * ns
    cap = 2 * rows // owners
    groups = nz // 2
    per = 2 * ns
    grows = per * cap
    vmem = pl.BlockSpec(memory_space=pltpu.VMEM)
    smem = pl.BlockSpec(memory_space=pltpu.SMEM)
    dma = pltpu.SemaphoreType.DMA
    return pl.pallas_call(
        functools.partial(block_kernel, sizes),
        out_shape=jax.ShapeDtypeStruct((rows, LANES), BF16),
        in_specs=[vmem, vmem, vmem, smem] + [vmem] * 7,
        out_specs=vmem,
        scratch_shapes=[
            pltpu.VMEM((rows, LANES), BF16),
            pltpu.VMEM((groups, per, cap, LANES), BF16),
            pltpu.VMEM((owners, 1, LANES), F32),
            pltpu.VMEM((groups, per, 1, LANES), F32),
            pltpu.VMEM((groups, per, cap, width), BF16),
            pltpu.VMEM((groups, grows, LANES), F32),
            pltpu.VMEM((rows, LANES), F32),
            pltpu.VMEM((WIN_DEV * WLEN, 3 * LANES), BF16),
            pltpu.VMEM((LANES, WIN_DEV * WLEN), BF16),
            pltpu.VMEM((groups, per, cap, LANES), BF16),
            pltpu.VMEM((groups, per, cap, LANES), BF16),
            pltpu.VMEM((LANES // HDIM, WLEN, WLEN), F32),
            pltpu.VMEM((LANES // HDIM, WLEN, WLEN), F32),
            pltpu.VMEM((groups, cap, width), BF16),
            pltpu.VMEM((groups, nm, cap, LANES), BF16),
            pltpu.VMEM((groups, nm, cap, LANES), BF16),
            pltpu.VMEM((groups, nm, cap, LANES), BF16),
            dma((groups, 2)),
            dma((groups, 2)),
            pltpu.VMEM((nm,) + wo.shape, BF16),
            pltpu.VMEM((nm,) + wu.shape, BF16),
            pltpu.VMEM((nm,) + wd.shape, BF16),
            dma((groups,)),
            dma((groups,)),
            dma((groups,)),
            dma((groups,)),
            dma((groups, 2)),
            dma((groups, 2)),
            dma((groups,)),
            dma((groups,)),
            dma((3, 2)),
            dma((3, 2)),
            dma((3, 2)),
            dma((3, 2)),
            dma((3, nm - 1)),
            dma((3, nm - 1)),
            dma((groups, nm - 1)),
            dma((groups, nm - 1)),
            dma((groups, nm - 1)),
            dma((groups, nm - 1)),
        ],
        compiler_params=pltpu.CompilerParams(
            collective_id=0, has_side_effects=True, vmem_limit_bytes=60 * 1024 * 1024
        ),
        name="block",
    )(
        x,
        ids,
        slots,
        counts,
        gain.reshape(1, width),
        wqk,
        wv,
        wo,
        fgain.reshape(1, width),
        wu,
        wd,
    )


def solution(mesh):
    sizes = (mesh.shape["space"], mesh.shape["mp"], mesh.shape["sub"])
    return jax.shard_map(
        functools.partial(shards, sizes),
        mesh=mesh,
        in_specs=(
            P(("groups", "space", "sub"), None),
            P(("groups", "space", "sub")),
            P(("groups", "space", "sub")),
            P("groups"),
            P(),
            P(None, None, "mp"),
            P(None, "mp"),
            P("mp", None),
            P(),
            P(None, "mp"),
            P("mp", None),
        ),
        out_specs=P(("groups", "space", "sub"), "mp"),
        check_vma=False,
    )
```
